256 devices in a mesh: section: 8 (over z), ep: 32 (over x, y, core).
Axes of the slice: x: 4, y: 4, z: 8, core: 2. Of those that a mesh axis runs over, the one named last changes fastest.
Arguments:
- saved_inputs: bfloat16 [8, 4096, 4096], P('section', 'ep'), may hold values from -6 to 6
- expert_ids: int32 [8, 4096, 2], P('section', 'ep'), may hold values from 0 to 7, as said below
- gate_weights: float32 [8, 4096, 2], P('section', 'ep'), may hold values from 0.1 to 0.9
- out_grad: bfloat16 [4096, 4096], P('ep', 'section'), may hold values from -6 to 6
- gate_w: bfloat16 [8, 7168, 4096], P('section', 'ep'), may hold values from -0.09375 to 0.09375
- up_w: bfloat16 [8, 7168, 4096], P('section', 'ep'), may hold values from -0.09375 to 0.09375
- down_w: bfloat16 [8, 7168, 4096], P('section', 'ep'), may hold values from -0.0625 to 0.0625
Outputs:
- input_grads: bfloat16 [8, 4096, 4096], P('section', 'ep')
- grad_gate: bfloat16 [8, 7168, 4096], P('section', 'ep')
- grad_up: bfloat16 [8, 7168, 4096], P('section', 'ep')
- grad_down: bfloat16 [8, 7168, 4096], P('section', 'ep')
The draws below stay inside these ranges and needn't reach their ends.
Inputs may be any that keep to these rules, and one draw needn't show every extreme that they name: `expert_ids`: the two ids of a token differ. Among the 128 tokens of one device in one layer, at most 4 name expert 0, and in every layer some device's tokens name it exactly 4 times.
All inputs are finite; a program needn't handle non-finite values.
Results may differ from the reference program's by a relative error of at most 0.0058.
Values may be sent and summed in bfloat16 or wider, within the bound.
No kernel may reach another device: no remote copies, remote signals or barrier semaphores. Data moves between devices by JAX's collectives and lax.ppermute only.
A program may use at most 128 MiB of HBM per device.

```python
import jax
import jax.numpy as jnp
from jax import lax

D = 4096
EXPERTS = 8
TOK_DEV = 128
CAP = 4
FFW = 7168
SECTIONS = 8
TOKENS = 4096
N_EP = 32


def draw_expert_ids(key, part):
    groups = TOKENS // TOK_DEV
    blocks = SECTIONS * groups
    keys = jax.random.split(key, 7)
    first_count = jax.random.randint(keys[0], (SECTIONS, groups), 1, CAP + 1)
    second_count = jax.random.randint(keys[1], (SECTIONS, groups), 1, CAP + 1)
    counts = jnp.minimum(first_count, second_count)
    fullest = jax.random.randint(keys[2], (SECTIONS, 1), 0, groups)
    counts = jnp.where(jnp.arange(groups)[None, :] == fullest, CAP, counts).reshape(blocks, 1)
    ranks = jax.vmap(lambda block_key: jax.random.permutation(block_key, TOK_DEV))(jax.random.split(keys[3], blocks))
    is_live = ranks < counts
    other_first = jax.random.randint(keys[4], (blocks, TOK_DEV), 1, EXPERTS)
    other_second = jax.random.randint(keys[5], (blocks, TOK_DEV), 1, EXPERTS - 1)
    other_second = other_second + (other_second >= other_first).astype(jnp.int32)
    which_side = jax.random.randint(keys[6], (blocks, TOK_DEV), 0, 2)
    id_zero = jnp.where(is_live, jnp.where(which_side == 0, 0, other_first), other_first)
    id_one = jnp.where(is_live, jnp.where(which_side == 0, other_first, 0), other_second)
    return jnp.stack([id_zero, id_one], -1).reshape(SECTIONS, TOKENS, 2).astype(jnp.int32)


def steps_of(key, shape, cuts, least, top_value):
    level, own = 1.0, jax.random.fold_in(key, 6)
    for dim, blocks in cuts:
        draws = jnp.exp(jax.random.uniform(jax.random.fold_in(own, dim), (blocks,), jnp.float32, least / len(cuts), top_value / len(cuts)))
        level = level * jnp.repeat(draws, shape[dim] // blocks).reshape([-1 if axis == dim else 1 for axis in range(len(shape))])
    return level


def gaussian(own_key, extent, scale, limit, cuts=(), held_as=jnp.bfloat16):
    values = scale * jax.random.normal(own_key, extent, jnp.float32)
    if cuts:
        values = values * steps_of(own_key, extent, cuts, -0.22, 0.18)
    return jnp.clip(values, -limit, limit).astype(held_as)


def setup_inputs(seed: int = 0) -> dict:
    key_list = jax.random.split(jax.random.key(seed), 8)
    return {
        "saved_inputs": gaussian(key_list[0], (SECTIONS, TOKENS, D), 1.0, 6.0, ((0, 8), (1, 32))),
        "expert_ids": draw_expert_ids(jax.random.fold_in(key_list[7], 71), 0),
        "gate_weights": jnp.clip(0.1 + 0.79999997 * jax.random.uniform(key_list[2], (SECTIONS, TOKENS, 2), jnp.float32) ** steps_of(key_list[2], (SECTIONS, TOKENS, 2), ((0, 8), (1, 32)), -0.2, 0.2), 0.1, 0.9),
        "out_grad": gaussian(key_list[3], (TOKENS, D), 1.0, 6.0, ((0, 32), (1, 8))),
        "gate_w": gaussian(key_list[4], (SECTIONS, FFW, D), D ** -0.5, 0.09375, ((0, 8), (1, 32))),
        "up_w": gaussian(key_list[5], (SECTIONS, FFW, D), D ** -0.5, 0.09375, ((0, 8), (1, 32))),
        "down_w": gaussian(key_list[6], (SECTIONS, FFW, D), FFW ** -0.5, 0.0625, ((0, 8), (1, 32))),
    }


def reference(saved_inputs, expert_ids, gate_weights, out_grad, gate_w, up_w, down_w):
    device_of = (jnp.arange(TOKENS, dtype=jnp.int32) // TOK_DEV).astype(jnp.int32)

    def section_backward(upstream, operands):
        tokens, routes, gate_share, w_gate, w_up, w_down = operands
        is_live = routes == 0
        live_count = jnp.sum(is_live.astype(jnp.int32), axis=1).astype(jnp.int32)
        pair_weight = jnp.sum(jnp.where(is_live, gate_share, 0.0), axis=1)
        per_device = live_count.reshape(N_EP, TOK_DEV)
        slot_index = (jnp.cumsum(per_device, axis=1) - per_device).reshape(TOKENS).astype(jnp.int32)
        target = (device_of * (CAP + 1) + jnp.where(live_count == 1, slot_index, CAP)).astype(jnp.int32)

        def pack_rows(row_data):
            buffer = jnp.zeros((N_EP * (CAP + 1), D), row_data.dtype).at[target].set(row_data)
            return buffer.reshape(N_EP, CAP + 1, D)[:, :CAP].reshape(N_EP * CAP, D)

        scaled = (pair_weight[:, None] * upstream.astype(jnp.float32)).astype(jnp.bfloat16)
        x_rows = pack_rows(tokens)
        y_rows = pack_rows(scaled)
        gate_pre = jnp.dot(x_rows, w_gate.T, preferred_element_type=jnp.float32)
        up_pre = jnp.dot(x_rows, w_up.T, preferred_element_type=jnp.float32)
        sigmoid_gate = jax.nn.sigmoid(gate_pre)
        activated = gate_pre * sigmoid_gate
        hidden = (activated * up_pre).astype(jnp.bfloat16)
        grad_hidden = jnp.dot(y_rows, w_down.T, preferred_element_type=jnp.float32)
        d_up = (grad_hidden * activated).astype(jnp.bfloat16)
        d_gate = (grad_hidden * up_pre * sigmoid_gate * (1.0 + gate_pre * (1.0 - sigmoid_gate))).astype(jnp.bfloat16)
        back_rows = (jnp.dot(d_gate, w_gate, preferred_element_type=jnp.float32)
                     + jnp.dot(d_up, w_up, preferred_element_type=jnp.float32))
        padded = jnp.concatenate([back_rows.reshape(N_EP, CAP, D),
                                  jnp.zeros((N_EP, 1, D), back_rows.dtype)], 1).reshape(N_EP * (CAP + 1), D)
        input_grad = (upstream.astype(jnp.float32) + padded[target]).astype(jnp.bfloat16)
        grad_gate = jnp.dot(d_gate.T, x_rows, preferred_element_type=jnp.float32).astype(jnp.bfloat16)
        grad_up = jnp.dot(d_up.T, x_rows, preferred_element_type=jnp.float32).astype(jnp.bfloat16)
        grad_down = jnp.dot(hidden.T, y_rows, preferred_element_type=jnp.float32).astype(jnp.bfloat16)
        return input_grad, (input_grad, grad_gate, grad_up, grad_down)

    final_grad, outputs = lax.scan(section_backward, out_grad,
                                   (saved_inputs, expert_ids, gate_weights, gate_w, up_w, down_w), reverse=True)
    return (outputs[0], outputs[1], outputs[2], outputs[3])
```

```python
import jax
import jax.numpy as jnp
from jax import lax
from jax.sharding import PartitionSpec as P

CAP = 4
FEW = 16
F32 = jnp.float32
BF16 = jnp.bfloat16


def same_core_groups(devices):
    return [[2 * chip + core for chip in range(devices // 2)] for core in range(2)]


def exchange(blocks, axis, groups=None):
    return lax.all_to_all(blocks, axis, 0, 0, tiled=True, axis_index_groups=groups)


def repeated(value, count):
    return jnp.broadcast_to(value[None], (count, *value.shape))


def from_partner(value, devices):
    return lax.ppermute(value, "ep", [(i, i ^ 1) for i in range(devices)])


def project(row_data, weight):
    return lax.dot_general(
        row_data, weight, (((1,), (1,)), ((), ())), preferred_element_type=F32
    )


def matmul(left, right):
    return jnp.dot(left, right, preferred_element_type=F32)


def sum_units(left, right):
    return lax.dot_general(
        left, right, (((0,), (0,)), ((), ())), preferred_element_type=F32
    )


def on_device(saved_inputs, expert_ids, gate_weights, out_grad, gate_w, up_w, down_w):
    sections = lax.axis_size("section")
    devices = lax.axis_size("ep")
    chips = devices // 2
    section = lax.axis_index("section")
    core = lax.axis_index("ep") % 2
    groups = same_core_groups(devices)
    width = saved_inputs.shape[2]
    columns = width // devices
    slots = devices * CAP
    tokens = saved_inputs[0]
    token_count = tokens.shape[0]
    is_live = expert_ids[0] == 0
    w_gate = gate_w[0]
    w_up = up_w[0]
    w_down = down_w[0]

    live_count = jnp.sum(is_live.astype(jnp.int32), axis=1)
    pair_weight = jnp.sum(jnp.where(is_live, gate_weights[0], 0.0), axis=1)
    slot_index = jnp.cumsum(live_count) - live_count
    target = jnp.where(live_count == 1, slot_index, CAP)
    chosen = target[None, :] == jnp.arange(CAP, dtype=jnp.int32)[:, None]
    selector = chosen.astype(BF16)
    token_index = jnp.arange(token_count, dtype=jnp.int32)
    slot_token = jnp.sum(jnp.where(chosen, token_index[None, :] + 1, 0), axis=1) - 1
    slot_weight = jnp.sum(jnp.where(chosen, pair_weight[None, :], 0.0), axis=1)

    note = jnp.zeros((8, out_grad.shape[1]), BF16)
    note = lax.dynamic_update_slice(note, slot_token.astype(BF16)[None], (0, 0))
    above = exchange(repeated(jnp.concatenate([out_grad, note], 0), sections), "section")
    upstream = above[:, :token_count]
    layer_tokens = above[:, token_count, :CAP]

    x_four = matmul(selector, tokens).astype(BF16)
    up_four = lax.dot_general(
        selector, upstream, (((1,), (1,)), ((), ())), preferred_element_type=F32
    ).reshape(CAP, width)
    y_four = (slot_weight[:, None] * up_four).astype(BF16)
    weight_high = slot_weight.astype(BF16)
    weight_low = (slot_weight - weight_high.astype(F32)).astype(BF16)
    extra = jnp.zeros((2 * CAP, 128), BF16)
    extra = lax.dynamic_update_slice(extra, layer_tokens, (0, 0))
    extra = lax.dynamic_update_slice(extra, weight_high[None], (0, CAP))
    extra = lax.dynamic_update_slice(extra, weight_low[None], (0, 2 * CAP))
    packed = jnp.concatenate([jnp.concatenate([x_four, y_four], 0), extra], 1)
    mine = exchange(repeated(packed, chips), "ep", groups)
    other = from_partner(mine, devices)
    both = jnp.stack([mine, other])
    x_rows = both[:, :, :CAP, :width].reshape(slots, width)
    y_first = both[:, :, CAP:, :width].reshape(slots, width)
    notes = both[:, :, :, width : width + 3 * CAP].astype(F32)

    gate_pre = project(x_rows, w_gate)
    up_pre = project(x_rows, w_up)
    sig = jax.nn.sigmoid(gate_pre)
    act = gate_pre * sig
    hidden = (act * up_pre).astype(BF16)
    slope = up_pre * sig * (1.0 + gate_pre * (1.0 - sig))
    grad_first = project(y_first, w_down)
    up_first = (grad_first * act).astype(BF16)
    gate_first = (grad_first * slope).astype(BF16)

    ordered = jnp.where(core == 0, notes, notes[::-1])
    ordered = jnp.swapaxes(ordered, 0, 1).reshape(devices, 2 * CAP, 3 * CAP)
    row_weight = (ordered[:, 0, CAP : 2 * CAP] + ordered[:, 0, 2 * CAP :]).reshape(slots)
    within = jnp.swapaxes(ordered[:, :, :CAP], 0, 1)
    base = jnp.arange(devices, dtype=jnp.int32)[None, :, None] * token_count
    token_of = jnp.where(within >= 0, within.astype(jnp.int32) + base, -1)
    same = (token_of[:, None, :, :, None] == token_of[None, :, :, None, :]) & (
        token_of[:, None, :, :, None] >= 0
    )
    shared = jnp.any(same, axis=4)
    times = jnp.sum(shared.astype(jnp.int32), axis=1)
    trips = jnp.max(times) - 1
    in_chain = (times > 1).reshape(sections, slots)
    flat_token = token_of.reshape(sections, slots)
    chain_count = jnp.sum(in_chain.astype(jnp.int32), axis=1)
    place = jnp.cumsum(in_chain.astype(jnp.int32), axis=1) - 1

    own_chain = lax.dynamic_index_in_dim(in_chain, section, 0, keepdims=False)
    own_place = lax.dynamic_index_in_dim(place, section, 0, keepdims=False)
    layer_index = jnp.arange(sections, dtype=jnp.int32)

    def local_order(by_slot):
        pairs = jnp.swapaxes(by_slot.reshape(chips, 2, CAP), 0, 1)
        return jnp.where(core == 0, pairs, pairs[::-1]).reshape(slots)

    chain_here = local_order(own_chain)
    place_here = local_order(own_place)

    def corrected(size):
        index = jnp.arange(size, dtype=jnp.int32)
        listed = in_chain[:, None, :] & (place[:, None, :] == index[None, :, None])
        list_token = jnp.sum(jnp.where(listed, flat_token[:, None, :] + 1, 0), axis=2) - 1
        own_token = lax.dynamic_index_in_dim(list_token, section, 0, keepdims=False)
        own_listed = lax.dynamic_index_in_dim(listed, section, 0, keepdims=False)
        list_weight = jnp.sum(jnp.where(own_listed, row_weight[None, :], 0.0), axis=1)
        feeds = (
            (own_token[:, None, None] == list_token[None])
            & (own_token[:, None, None] >= 0)
            & (layer_index[None, :, None] > section)
        )
        feeds = feeds.reshape(size, sections * size).astype(BF16)
        pick = (chain_here[None, :] & (place_here[None, :] == index[:, None])).astype(BF16)
        act_few = jnp.dot(pick.astype(F32), act, precision=lax.Precision.HIGHEST)
        slope_few = jnp.dot(pick.astype(F32), slope, precision=lax.Precision.HIGHEST)
        y_few = matmul(pick, y_first)

        def more(state):
            return state[0] < trips

        def step(state):
            trip, _, d_gate, d_up = state
            share = (matmul(d_gate, w_gate) + matmul(d_up, w_up)).astype(BF16)
            share = jnp.swapaxes(share.reshape(size, devices, columns), 0, 1)
            summed = jnp.sum(exchange(share, "ep").astype(F32), axis=0).astype(BF16)
            layers = exchange(repeated(summed, sections), "section")
            added = matmul(feeds, layers.reshape(sections * size, columns))
            added = (list_weight[:, None] * added).astype(BF16)
            added = exchange(repeated(added, devices), "ep")
            added = jnp.swapaxes(added, 0, 1).reshape(size, width)
            grad_few = project((y_few + added.astype(F32)).astype(BF16), w_down)
            return (
                trip + 1,
                added,
                (grad_few * slope_few).astype(BF16),
                (grad_few * act_few).astype(BF16),
            )

        start = (
            jnp.int32(0),
            jnp.zeros((size, width), BF16),
            matmul(pick, gate_first).astype(BF16),
            matmul(pick, up_first).astype(BF16),
        )
        _, added, d_gate, d_up = lax.while_loop(more, step, start)
        y_rows = (y_first.astype(F32) + sum_units(pick, added)).astype(BF16)
        keep = jnp.logical_not(chain_here)[:, None]
        return (
            y_rows,
            jnp.where(keep, gate_first, sum_units(pick, d_gate).astype(BF16)),
            jnp.where(keep, up_first, sum_units(pick, d_up).astype(BF16)),
        )

    y_rows, d_gate, d_up = lax.cond(
        jnp.max(chain_count) <= FEW,
        lambda: corrected(FEW),
        lambda: corrected(slots),
    )

    back = (matmul(d_gate, w_gate) + matmul(d_up, w_up)).astype(BF16)
    half = slots // 2
    theirs = from_partner(back[half:], devices)
    chip_sum = (back[:half].astype(F32) + theirs.astype(F32)).astype(BF16)
    tiles = exchange(chip_sum.reshape(chips, CAP, width), "ep", groups)
    back_four = jnp.sum(tiles.astype(F32), axis=0).astype(BF16)
    all_back = exchange(repeated(back_four, sections), "section")
    takes = (
        (layer_tokens.astype(jnp.int32)[:, :, None] == token_index[None, None, :])
        & (layer_index[:, None, None] >= section)
    )
    takes = takes.reshape(sections * CAP, token_count).astype(BF16)
    whole = jnp.swapaxes(upstream, 0, 1).reshape(token_count, width)
    result = whole.astype(F32) + sum_units(takes, all_back.reshape(sections * CAP, width))

    return (
        result.astype(BF16)[None],
        sum_units(d_gate, x_rows).astype(BF16)[None],
        sum_units(d_up, x_rows).astype(BF16)[None],
        sum_units(hidden, y_rows).astype(BF16)[None],
    )


def solution(mesh):
    by_rows = P("section", "ep", None)
    return jax.shard_map(
        on_device,
        mesh=mesh,
        in_specs=(by_rows, by_rows, by_rows, P("ep", "section"), by_rows, by_rows, by_rows),
        out_specs=(by_rows, by_rows, by_rows, by_rows),
        check_vma=False,
    )
```

```python
import jax
import jax.numpy as jnp
from jax import lax
from jax.experimental import pallas as pl
from jax.experimental.pallas import tpu as pltpu
from jax.sharding import PartitionSpec as P

CAP = 4
ROWS = 2 * CAP
FEW = 16
LANES = 128
F32 = jnp.float32
BF16 = jnp.bfloat16


def exchange(blocks, axis, groups=None):
    return lax.all_to_all(blocks, axis, 0, 0, tiled=True, axis_index_groups=groups)


def repeated(value, count):
    return jnp.broadcast_to(value[None], (count, *value.shape))


def from_partner(value, devices):
    return lax.ppermute(value, "ep", [(i, i ^ 1) for i in range(devices)])


def project(row_data, weight):
    return lax.dot_general(
        row_data, weight, (((1,), (1,)), ((), ())), preferred_element_type=F32
    )


def matmul(left, right):
    return jnp.dot(left, right, preferred_element_type=F32)


def sum_rows(left, right):
    return lax.dot_general(
        left, right, (((0,), (0,)), ((), ())), preferred_element_type=F32
    )


def iota(shape, dim):
    return lax.broadcasted_iota(jnp.int32, shape, dim)


def chain_plan(where, mine, other, width, sections, slots):
    half = mine.shape[0] // ROWS
    devices = 2 * half
    codes = sections * CAP

    def kernel(where_ref, mine_ref, other_ref, feeds_ref, pick_ref, weight_ref, note_ref, count_ref):
        section = where_ref[0]
        core = where_ref[1]
        as_float = lambda mask: jnp.where(mask, 1.0, 0.0)
        lead = as_float(iota((half, half * ROWS), 1) == ROWS * iota((half, half * ROWS), 0)).astype(BF16)
        near = matmul(lead, mine_ref[...])
        far = matmul(lead, other_ref[...])
        note = jnp.concatenate([jnp.where(core == 0, near, far), jnp.where(core == 0, far, near)], 0)
        note_ref[...] = note
        lane = iota((devices, LANES), 1)
        code = jnp.where(lane < codes, note, -1.0)
        flag = as_float(code >= 0)
        row = iota((LANES, LANES), 0)
        col = iota((LANES, LANES), 1)
        same_layer = row // CAP == col // CAP
        per_layer = matmul(flag, as_float(same_layer))
        count_ref[0] = jnp.max(jnp.sum(per_layer, axis=0, keepdims=True)).astype(jnp.int32)
        most = jnp.max(jnp.where(lane == codes + 2 * CAP, note, 0.0))
        count_ref[1] = most.astype(jnp.int32) - 1
        before = as_float(iota((devices, devices), 1) < iota((devices, devices), 0))
        rank = matmul(before, per_layer) + matmul(flag, as_float(same_layer & (row < col)))
        rank = (rank + 1.0) * flag
        token = (code + 1.0) * flag
        owned = as_float(iota((8, LANES), 1) == iota((8, LANES), 0) + CAP * section)
        own_rank = project(owned, rank)
        own_token = project(owned, token)
        entry = iota((FEW, devices), 0).astype(F32) + 1.0
        device = iota((devices, 2 * LANES), 0)
        spot = iota((devices, 2 * LANES), 1)
        home = LANES * ((device // half + core) % 2) + ROWS * (device % half)
        held = jnp.zeros((FEW, 1), F32)
        weight = jnp.zeros((FEW, LANES), F32)
        groups = jnp.zeros((FEW, devices), F32)
        pick = jnp.zeros((FEW, 2 * LANES), F32)
        few_lane = iota((FEW, LANES), 1)
        for slot in range(CAP):
            here = as_float(own_rank[slot : slot + 1] == entry)
            groups = groups + here
            held = held + jnp.sum(here * own_token[slot : slot + 1], axis=1, keepdims=True)
            part = matmul(here, note)
            wanted = (few_lane == codes + slot) | (few_lane == codes + CAP + slot)
            weight = weight + jnp.where(wanted, part, 0.0)
            pick = pick + matmul(here, as_float(spot == home + slot))
        near_rank = matmul(groups, rank)
        near_token = matmul(groups, token)
        match = (near_token == held) & (near_token > 0) & (few_lane // CAP > section)
        source = jnp.where(match & (few_lane < codes), near_rank, 0.0)
        feeds = jnp.zeros((FEW, LANES), F32)
        for slot in range(CAP):
            spread = as_float((row // CAP == col // FEW) & (row % CAP == slot))
            feeds = feeds + as_float(
                matmul(source, spread) == (few_lane % FEW + 1).astype(F32)
            )
        feeds_ref[...] = feeds.astype(BF16)
        pick_ref[...] = pick.astype(BF16)
        weight_ref[...] = jnp.broadcast_to(
            jnp.sum(weight, axis=1, keepdims=True), (FEW, LANES)
        )

    inside = lambda rows, lanes: pl.BlockSpec((rows, lanes), lambda i: (0, 0))
    tile = pl.BlockSpec((half * ROWS, LANES), lambda i: (0, width // LANES))
    return pl.pallas_call(
        kernel,
        grid=(1,),
        in_specs=[pl.BlockSpec(memory_space=pltpu.SMEM), tile, tile],
        out_specs=[
            inside(FEW, sections * FEW),
            inside(FEW, ROWS * devices),
            inside(FEW, LANES),
            inside(devices, LANES),
            pl.BlockSpec(memory_space=pltpu.SMEM),
        ],
        out_shape=[
            jax.ShapeDtypeStruct((FEW, sections * FEW), BF16),
            jax.ShapeDtypeStruct((FEW, ROWS * devices), BF16),
            jax.ShapeDtypeStruct((FEW, LANES), F32),
            jax.ShapeDtypeStruct((devices, LANES), F32),
            jax.ShapeDtypeStruct((2,), jnp.int32),
        ],
    )(where, mine, other)


def weight_gradients(mine, other, d_gate, d_up, hidden, hidden_few, added, width):
    units = d_gate.shape[1]
    block = 512
    half = mine.shape[0]
    few = added.shape[0]

    def kernel(mine_ref, other_ref, dg_ref, du_ref, h_ref, hf_ref, added_ref, gate_out, up_out, down_out):
        first = mine_ref[...]
        second = other_ref[...]

        def both(ref):
            return sum_rows(ref[:half], first) + sum_rows(ref[half:], second)

        gate_out[...] = both(dg_ref).astype(BF16)
        up_out[...] = both(du_ref).astype(BF16)
        down_out[...] = (both(h_ref) + sum_rows(hf_ref[...], added_ref[...])).astype(BF16)

    columns = lambda rows: pl.BlockSpec((rows, block), lambda i: (0, i))
    whole = lambda value: pl.BlockSpec(value.shape, lambda i: (0, 0))
    return pl.pallas_call(
        kernel,
        grid=(width // block,),
        in_specs=[
            columns(half),
            columns(half),
            whole(d_gate),
            whole(d_up),
            whole(hidden),
            whole(hidden_few),
            columns(few),
        ],
        out_specs=[columns(units)] * 3,
        out_shape=[jax.ShapeDtypeStruct((units, width), BF16)] * 3,
    )(mine, other, d_gate, d_up, hidden, hidden_few, added)


def on_device(saved_inputs, expert_ids, gate_weights, out_grad, gate_w, up_w, down_w):
    sections = lax.axis_size("section")
    devices = lax.axis_size("ep")
    chips = devices // 2
    section = lax.axis_index("section")
    core = lax.axis_index("ep") % 2
    groups = [[2 * chip + k for chip in range(chips)] for k in range(2)]
    width = saved_inputs.shape[2]
    columns = width // devices
    slots = devices * CAP
    tokens = saved_inputs[0]
    token_count = tokens.shape[0]
    is_live = expert_ids[0] == 0
    w_gate = gate_w[0]
    w_up = up_w[0]
    w_down = down_w[0]

    live_count = jnp.sum(is_live.astype(jnp.int32), axis=1)
    pair_weight = jnp.sum(jnp.where(is_live, gate_weights[0], 0.0), axis=1)
    slot_index = jnp.cumsum(live_count) - live_count
    target = jnp.where(live_count == 1, slot_index, CAP)
    chosen = target[None, :] == jnp.arange(CAP, dtype=jnp.int32)[:, None]
    selector = chosen.astype(BF16)
    token_index = jnp.arange(token_count, dtype=jnp.int32)
    slot_token = jnp.sum(jnp.where(chosen, token_index[None, :] + 1, 0), axis=1) - 1
    slot_weight = jnp.sum(jnp.where(chosen, pair_weight[None, :], 0.0), axis=1)
    x_four = matmul(selector, tokens).astype(BF16)

    note = jnp.zeros((8, out_grad.shape[1]), BF16)
    note = lax.dynamic_update_slice(note, slot_token.astype(BF16)[None], (0, 0))
    weight_high = slot_weight.astype(BF16)
    weight_low = (slot_weight - weight_high.astype(F32)).astype(BF16)
    where = jnp.stack([section, core]).astype(jnp.int32)
    sent, x_four, slot_weight, selector, weight_high, weight_low, where = lax.optimization_barrier(
        (
            repeated(jnp.concatenate([out_grad, note], 0), sections),
            x_four,
            slot_weight,
            selector,
            weight_high,
            weight_low,
            where,
        )
    )
    above = exchange(sent, "section")
    upstream = above[:, :token_count]
    layer_tokens = above[:, token_count, :CAP].astype(jnp.int32)

    equal = layer_tokens[:, :, None, None] == layer_tokens[None, None]
    times = jnp.sum(equal.astype(jnp.int32), axis=(2, 3))
    times = jnp.where(layer_tokens >= 0, times, 0)
    code = jnp.where(times > 1, layer_tokens, -1).reshape(1, sections * CAP)

    up_four = lax.dot_general(
        selector, upstream, (((1,), (1,)), ((), ())), preferred_element_type=F32
    ).reshape(CAP, width)
    y_four = (slot_weight[:, None] * up_four).astype(BF16)
    extra = jnp.concatenate(
        [
            code.astype(BF16),
            weight_high[None],
            weight_low[None],
            jnp.max(times).astype(BF16).reshape(1, 1),
            jnp.zeros((1, LANES - (sections + 2) * CAP - 1), BF16),
        ],
        1,
    )
    extra = jnp.broadcast_to(extra, (ROWS, LANES))
    packed = jnp.concatenate([jnp.concatenate([x_four, y_four], 0), extra], 1)
    packed, above, layer_tokens = lax.optimization_barrier(
        (repeated(packed, chips), above, layer_tokens)
    )
    arrived = exchange(packed, "ep", groups)
    partner = from_partner(arrived, devices)
    mine = arrived.reshape(chips * ROWS, width + LANES)
    other = partner.reshape(chips * ROWS, width + LANES)

    x_row = (jnp.arange(chips * ROWS) % ROWS < CAP)[:, None]

    def forward(rows):
        row_data = rows[:, :width]
        gate_pre = project(row_data, w_gate)
        up_pre = project(row_data, w_up)
        grad = jnp.roll(project(row_data, w_down), -CAP, axis=0)
        sig = jax.nn.sigmoid(gate_pre)
        act = gate_pre * sig
        slope = up_pre * sig * (1.0 + gate_pre * (1.0 - sig))
        only = lambda value: jnp.where(x_row, value, 0.0)
        return (
            only(act),
            only(slope),
            only(act * up_pre).astype(BF16),
            only(grad * slope).astype(BF16),
            only(grad * act).astype(BF16),
        )

    pairs = zip(forward(mine), forward(other))
    act, slope, hidden, gate_first, up_first = (jnp.concatenate(pair, 0) for pair in pairs)

    feeds_few, pick_few, weight_few, notes, counts = chain_plan(
        where, mine, other, width, sections, slots
    )
    trips = counts[1]
    chain_count = counts[0]
    layer_index = jnp.arange(sections, dtype=jnp.int32)

    def slow_plan(size):
        index = jnp.arange(size, dtype=jnp.int32)
        in_chain = (notes[:, : sections * CAP] >= 0).reshape(devices, sections, CAP)
        flags = jnp.swapaxes(in_chain, 0, 1).reshape(sections, slots)
        within = notes[:, : sections * CAP].astype(jnp.int32).reshape(devices, sections, CAP)
        base = token_count * jnp.arange(devices, dtype=jnp.int32)[:, None, None]
        token = jnp.swapaxes(within + base + 1, 0, 1).reshape(sections, slots)
        place = jnp.cumsum(flags.astype(jnp.int32), axis=1) - 1
        listed = flags[:, None, :] & (place[:, None, :] == index[None, :, None])
        tokens_of = jnp.sum(jnp.where(listed, token[:, None, :], 0), axis=2)
        own_token = lax.dynamic_index_in_dim(tokens_of, section, 0, keepdims=False)
        own = lax.dynamic_index_in_dim(listed, section, 0, keepdims=False)
        high = notes[:, sections * CAP : (sections + 1) * CAP]
        low = notes[:, (sections + 1) * CAP : (sections + 2) * CAP]
        weight = jnp.sum(jnp.where(own, (high + low).reshape(1, slots), 0.0), axis=1)
        feeds = (
            (own_token[:, None, None] == tokens_of[None])
            & (own_token[:, None, None] > 0)
            & (layer_index[None, :, None] > section)
        )
        halves = own.reshape(size, 2, chips, CAP)
        halves = jnp.where(core == 0, halves, halves[:, ::-1])
        halves = jnp.concatenate([halves, jnp.zeros_like(halves)], 3)
        return (
            feeds.reshape(size, sections * size).astype(BF16),
            halves.reshape(size, devices * ROWS).astype(BF16),
            jnp.broadcast_to(weight[:, None], (size, LANES)),
        )

    def finish(size):
        if size == FEW:
            feeds, pick, list_weight = feeds_few, pick_few, weight_few
        else:
            feeds, pick, list_weight = slow_plan(size)
        half = chips * ROWS
        exact = lax.Precision.HIGHEST
        act_few = jnp.dot(pick.astype(F32), act, precision=exact)
        slope_few = jnp.dot(pick.astype(F32), slope, precision=exact)
        y_pick = jnp.roll(pick, CAP, axis=1)
        y_few = matmul(y_pick[:, :half], mine[:, :width]) + matmul(y_pick[:, half:], other[:, :width])

        def more(state):
            return state[0] < trips

        def step(state):
            trip, _, d_gate, d_up = state
            share = (matmul(d_gate, w_gate) + matmul(d_up, w_up)).astype(BF16)
            share = jnp.swapaxes(share.reshape(size, devices, columns), 0, 1)
            share, trip = lax.optimization_barrier((share, trip + 1))
            summed = jnp.sum(exchange(share, "ep").astype(F32), axis=0).astype(BF16)
            layers = exchange(repeated(summed, sections), "section")
            added = matmul(feeds, layers.reshape(sections * size, columns))
            added = (list_weight * added).astype(BF16)
            added = exchange(repeated(added, devices), "ep")
            added = jnp.swapaxes(added, 0, 1).reshape(size, width)
            grad_few = project((y_few + added.astype(F32)).astype(BF16), w_down)
            return (
                trip,
                added,
                (grad_few * slope_few).astype(BF16),
                (grad_few * act_few).astype(BF16),
            )

        start = (
            jnp.int32(0),
            jnp.zeros((size, width), BF16),
            matmul(pick, gate_first).astype(BF16),
            matmul(pick, up_first).astype(BF16),
        )
        _, added, gate_few, up_few = lax.while_loop(more, step, start)
        keep = sum_rows(pick, jnp.ones((size, 1), BF16)) == 0.0
        d_gate = jnp.where(keep, gate_first, sum_rows(pick, gate_few).astype(BF16))
        d_up = jnp.where(keep, up_first, sum_rows(pick, up_few).astype(BF16))

        def x_only(value):
            return value.reshape(chips, ROWS, -1)[:, :CAP].reshape(chips * CAP, -1)

        def back(part):
            return (
                matmul(x_only(d_gate[part]), w_gate) + matmul(x_only(d_up[part]), w_up)
            ).astype(BF16)

        theirs = from_partner(back(slice(half, None)), devices)
        chip_sum = (back(slice(0, half)).astype(F32) + theirs.astype(F32)).astype(BF16)
        tiles = exchange(chip_sum.reshape(chips, CAP, width), "ep", groups)
        back_four = jnp.sum(tiles.astype(F32), axis=0).astype(BF16)
        all_back = exchange(repeated(back_four, sections), "section")
        takes = (layer_tokens[:, :, None] == token_index[None, None, :]) & (
            layer_index[:, None, None] >= section
        )
        takes = takes.reshape(sections * CAP, token_count).astype(BF16)
        whole = jnp.swapaxes(above[:, :token_count], 0, 1).reshape(token_count, width)
        result = whole.astype(F32) + sum_rows(takes, all_back.reshape(sections * CAP, width))
        grads = weight_gradients(
            mine,
            other,
            d_gate,
            d_up,
            jnp.roll(hidden, CAP, axis=0),
            matmul(pick, hidden).astype(BF16),
            added,
            width,
        )
        return (result.astype(BF16), *grads)

    outputs = lax.cond(chain_count <= FEW, lambda: finish(FEW), lambda: finish(slots))
    return tuple(output[None] for output in outputs)


def solution(mesh):
    by_rows = P("section", "ep", None)
    return jax.shard_map(
        on_device,
        mesh=mesh,
        in_specs=(by_rows, by_rows, by_rows, P("ep", "section"), by_rows, by_rows, by_rows),
        out_specs=(by_rows, by_rows, by_rows, by_rows),
        check_vma=False,
    )
```

```python
import jax
import jax.numpy as jnp
from jax import lax
from jax.experimental import pallas as pl
from jax.experimental.pallas import tpu as pltpu
from jax.sharding import PartitionSpec as P

CAP = 4
ROWS = 2 * CAP
FEW = 16
PARTS = 3
LANES = 128
F32 = jnp.float32
BF16 = jnp.bfloat16


def exchange(blocks, axis, groups=None):
    return lax.all_to_all(blocks, axis, 0, 0, tiled=True, axis_index_groups=groups)


def repeated(value, count):
    return jnp.broadcast_to(value[None], (count, *value.shape))


def from_partner(value, devices):
    return lax.ppermute(value, "ep", [(i, i ^ 1) for i in range(devices)])


def project(row_data, weight):
    return lax.dot_general(
        row_data, weight, (((1,), (1,)), ((), ())), preferred_element_type=F32
    )


def matmul(left, right):
    return jnp.dot(left, right, preferred_element_type=F32)


def sum_rows(left, right):
    return lax.dot_general(
        left, right, (((0,), (0,)), ((), ())), preferred_element_type=F32
    )


def iota(shape, dim):
    return lax.broadcasted_iota(jnp.int32, shape, dim)


def as_float(mask):
    return jnp.where(mask, 1.0, 0.0)


def start_copies(sources, targets, sems):
    copies = [
        pltpu.make_async_copy(source, target, sems.at[i])
        for i, (source, target) in enumerate(zip(sources, targets))
    ]
    for copy in copies:
        copy.start()
    return copies


def whole_spec(shape):
    return pl.BlockSpec(shape, lambda: (0,) * len(shape))


def weight_scratch(weight, count):
    return [pltpu.VMEM(weight.shape, BF16)] * count + [pltpu.SemaphoreType.DMA((count,))]


def first_pass(where, mine, other, w_gate, w_up, w_down, sections):
    half = mine.shape[0] // ROWS
    rows = half * ROWS
    devices = 2 * half
    codes = sections * CAP
    ending = codes + PARTS * CAP
    units, width = w_gate.shape
    columns = width // devices

    def kernel(
        where_ref,
        mine_ref,
        other_ref,
        gate_hbm,
        up_hbm,
        down_hbm,
        feeds_ref,
        pick_ref,
        weight_ref,
        note_ref,
        scale_ref,
        act_ref,
        slope_ref,
        hidden_ref,
        gate_ref,
        up_ref,
        act_few_ref,
        slope_few_ref,
        hidden_few_ref,
        gate_few_ref,
        up_few_ref,
        rows_few_ref,
        y_few_ref,
        share_ref,
        count_ref,
        w_gate_ref,
        w_up_ref,
        w_down_ref,
        sems,
    ):
        copies = start_copies(
            (down_hbm, gate_hbm, up_hbm), (w_down_ref, w_gate_ref, w_up_ref), sems
        )
        section = where_ref[0]
        core = where_ref[1]
        place = where_ref[2]

        lead = as_float(iota((half, rows), 1) == ROWS * iota((half, rows), 0)).astype(BF16)
        tiles = [ref[:, width:] for ref in (mine_ref, other_ref)]
        near = matmul(lead, tiles[0])
        far = matmul(lead, tiles[1])
        note = jnp.concatenate([jnp.where(core == 0, near, far), jnp.where(core == 0, far, near)], 0)
        note_ref[...] = note
        lane = iota((devices, LANES), 1)
        code = jnp.where(lane < codes, note, -1.0)
        flag = as_float(code >= 0)
        row = iota((LANES, LANES), 0)
        col = iota((LANES, LANES), 1)
        same_layer = row // CAP == col // CAP
        per_layer = matmul(flag, as_float(same_layer))
        count_ref[0] = jnp.max(jnp.sum(per_layer, axis=0, keepdims=True)).astype(jnp.int32)
        most = jnp.max(jnp.where(lane == codes + PARTS * CAP, note, 0.0))
        count_ref[1] = most.astype(jnp.int32) - 1
        before = as_float(iota((devices, devices), 1) < iota((devices, devices), 0))
        rank = matmul(before, per_layer) + matmul(flag, as_float(same_layer & (row < col)))
        rank = (rank + 1.0) * flag
        token = (code + 1.0) * flag
        owned = as_float(iota((8, LANES), 1) == iota((8, LANES), 0) + CAP * section)
        own_rank = project(owned, rank)
        own_token = project(owned, token)
        entry = iota((FEW, devices), 0).astype(F32) + 1.0
        device = iota((devices, 2 * rows), 0)
        spot = iota((devices, 2 * rows), 1)
        home = rows * ((device // half + core) % 2) + ROWS * (device % half)
        held = jnp.zeros((FEW, 1), F32)
        weight = jnp.zeros((FEW, LANES), F32)
        groups = jnp.zeros((FEW, devices), F32)
        pick = jnp.zeros((FEW, 2 * rows), F32)
        few_lane = iota((FEW, LANES), 1)
        for slot in range(CAP):
            here = as_float(own_rank[slot : slot + 1] == entry)
            groups = groups + here
            held = held + jnp.sum(here * own_token[slot : slot + 1], axis=1, keepdims=True)
            part = matmul(here, note)
            wanted = (few_lane >= codes) & (few_lane < ending) & (few_lane % CAP == slot)
            weight = weight + jnp.where(wanted, part, 0.0)
            pick = pick + matmul(here, as_float(spot == home + slot))
        near_rank = matmul(groups, rank)
        near_token = matmul(groups, token)
        match = (near_token == held) & (near_token > 0) & (few_lane // CAP > section)
        source = jnp.where(match & (few_lane < codes), near_rank, 0.0)
        feeds = jnp.zeros((FEW, LANES), F32)
        for slot in range(CAP):
            spread = as_float((row // CAP == col // FEW) & (row % CAP == slot))
            feeds = feeds + as_float(
                matmul(source, spread) == (few_lane % FEW + 1).astype(F32)
            )
        feeds_ref[...] = feeds.astype(BF16)
        pick_low = pick.astype(BF16)
        pick_ref[...] = pick_low
        weight_ref[...] = jnp.broadcast_to(
            jnp.sum(weight, axis=1, keepdims=True), (FEW, LANES)
        )

        kind = iota((rows, LANES), 0) % ROWS - CAP
        tile_lane = iota((rows, LANES), 1)
        wanted = (tile_lane >= codes) & (tile_lane < ending) & (tile_lane % CAP == kind)
        halves = []
        for index, ref in enumerate((mine_ref, other_ref)):
            scale = jnp.sum(
                jnp.where(wanted, tiles[index].astype(F32), 0.0), axis=1, keepdims=True
            )
            scale = jnp.where(kind[:, :1] >= 0, scale, 1.0)
            scale_ref[index * rows : (index + 1) * rows, :] = jnp.broadcast_to(scale, (rows, LANES))
            halves.append((ref[:, :width].astype(F32) * scale).astype(BF16))
        y_pick = pltpu.roll(pick, CAP, 1).astype(BF16)
        y_few_ref[...] = (
            matmul(y_pick[:, :rows], halves[0]) + matmul(y_pick[:, rows:], halves[1])
        ).astype(BF16)
        spot = pl.ds(pl.multiple_of(place * columns, columns), columns)
        rows_few_ref[...] = matmul(y_pick[:, :rows], mine_ref[:, spot]) + matmul(
            y_pick[:, rows:], other_ref[:, spot]
        )
        x_lane = iota((units, rows), 1) % ROWS < CAP
        copies[0].wait()
        grads = [
            pltpu.roll(project(w_down_ref[...], value), rows - CAP, 1) for value in halves
        ]
        copies[1].wait()
        gates = [project(w_gate_ref[...], value) for value in halves]
        copies[2].wait()
        for index in range(2):
            part = slice(index * rows, (index + 1) * rows)
            gate_pre = gates[index]
            up_pre = project(w_up_ref[...], halves[index])
            sig = 1.0 / (1.0 + jnp.exp(-gate_pre))
            act = jnp.where(x_lane, gate_pre * sig, 0.0)
            slope = jnp.where(x_lane, up_pre * sig * (1.0 + gate_pre * (1.0 - sig)), 0.0)
            act_ref[:, part] = act
            slope_ref[:, part] = slope
            hidden_ref[:, part] = (act * up_pre).astype(BF16)
            gate_ref[:, part] = (grads[index] * slope).astype(BF16)
            up_ref[:, part] = (grads[index] * act).astype(BF16)

        def exact(value):
            return lax.dot_general(
                value,
                pick,
                (((1,), (1,)), ((), ())),
                precision=lax.Precision.HIGHEST,
                preferred_element_type=F32,
            )

        act_few_ref[...] = exact(act_ref[...])
        slope_few_ref[...] = exact(slope_ref[...])
        hidden_few_ref[...] = project(hidden_ref[...], pick_low).astype(BF16)
        gate_few = project(gate_ref[...], pick_low).astype(BF16)
        up_few = project(up_ref[...], pick_low).astype(BF16)
        gate_few_ref[...] = gate_few
        up_few_ref[...] = up_few
        share = (sum_rows(gate_few, w_gate_ref[...]) + sum_rows(up_few, w_up_ref[...])).astype(BF16)
        for index in range(devices):
            share_ref[index] = share[:, index * columns : (index + 1) * columns]

    shapes = [
        ((FEW, sections * FEW), BF16),
        ((FEW, ROWS * devices), BF16),
        ((FEW, LANES), F32),
        ((devices, LANES), F32),
        ((2 * rows, LANES), F32),
        ((units, 2 * rows), F32),
        ((units, 2 * rows), F32),
        ((units, 2 * rows), BF16),
        ((units, 2 * rows), BF16),
        ((units, 2 * rows), BF16),
        ((units, FEW), F32),
        ((units, FEW), F32),
        ((units, FEW), BF16),
        ((units, FEW), BF16),
        ((units, FEW), BF16),
        ((FEW, columns), F32),
        ((FEW, width), BF16),
        ((devices, FEW, columns), BF16),
    ]
    smem = pl.BlockSpec(memory_space=pltpu.SMEM)
    anywhere = pl.BlockSpec(memory_space=pl.ANY)
    return pl.pallas_call(
        kernel,
        in_specs=[smem, whole_spec(mine.shape), whole_spec(other.shape)] + [anywhere] * 3,
        out_specs=[whole_spec(shape) for shape, _ in shapes] + [smem],
        out_shape=[jax.ShapeDtypeStruct(shape, dtype) for shape, dtype in shapes]
        + [jax.ShapeDtypeStruct((2,), jnp.int32)],
        scratch_shapes=weight_scratch(w_gate, 3),
    )(where, mine, other, w_gate, w_up, w_down)


def chain_step(y_blocks, act_few, slope_few, w_gate, w_up, w_down):
    devices, size, columns = y_blocks.shape
    units, width = w_gate.shape

    def kernel(
        blocks_ref,
        act_ref,
        slope_ref,
        gate_hbm,
        up_hbm,
        down_hbm,
        y_ref,
        gate_few_ref,
        up_few_ref,
        share_ref,
        w_gate_ref,
        w_up_ref,
        w_down_ref,
        sems,
    ):
        copies = start_copies(
            (down_hbm, gate_hbm, up_hbm), (w_down_ref, w_gate_ref, w_up_ref), sems
        )
        for index in range(devices):
            y_ref[:, index * columns : (index + 1) * columns] = blocks_ref[index]
        copies[0].wait()
        grad = project(w_down_ref[...], y_ref[...])
        gate_few = (grad * slope_ref[...]).astype(BF16)
        up_few = (grad * act_ref[...]).astype(BF16)
        gate_few_ref[...] = gate_few
        up_few_ref[...] = up_few
        copies[1].wait()
        share = sum_rows(gate_few, w_gate_ref[...])
        copies[2].wait()
        share = (share + sum_rows(up_few, w_up_ref[...])).astype(BF16)
        for index in range(devices):
            share_ref[index] = share[:, index * columns : (index + 1) * columns]

    shapes = [(size, width), (units, size), (units, size), (devices, size, columns)]
    anywhere = pl.BlockSpec(memory_space=pl.ANY)
    return pl.pallas_call(
        kernel,
        in_specs=[whole_spec(value.shape) for value in (y_blocks, act_few, slope_few)]
        + [anywhere] * 3,
        out_specs=[whole_spec(shape) for shape in shapes],
        out_shape=[jax.ShapeDtypeStruct(shape, BF16) for shape in shapes],
        scratch_shapes=weight_scratch(w_gate, 3),
    )(y_blocks, act_few, slope_few, w_gate, w_up, w_down)


def merge_chains(pick, gate, up, hidden, gate_few, up_few, w_gate, w_up):
    units, width = w_gate.shape
    lanes = gate.shape[1]
    rows = lanes // 2

    def kernel(
        pick_ref,
        gate_ref,
        up_ref,
        hidden_ref,
        gate_few_ref,
        up_few_ref,
        gate_hbm,
        up_hbm,
        gate_out,
        up_out,
        hidden_out,
        mine_out,
        other_out,
        w_gate_ref,
        w_up_ref,
        sems,
    ):
        copies = start_copies((gate_hbm, up_hbm), (w_gate_ref, w_up_ref), sems)
        pick_low = pick_ref[...]
        keep = jnp.sum(pick_low.astype(F32), axis=0, keepdims=True) == 0.0
        gate_all = jnp.where(keep, gate_ref[...].astype(F32), matmul(gate_few_ref[...], pick_low))
        up_all = jnp.where(keep, up_ref[...].astype(F32), matmul(up_few_ref[...], pick_low))
        gate_out[...] = gate_all.astype(BF16)
        up_out[...] = up_all.astype(BF16)
        kept = jnp.where(keep, hidden_ref[...].astype(F32), 0.0)
        hidden_out[...] = pltpu.roll(kept, CAP, 1).astype(BF16)
        side = width // 2

        def shares(value, ref, part):
            low = value[:, part]
            moved = pltpu.roll(low, CAP, 1)
            return sum_rows(low.astype(BF16), ref[:, :side]) + sum_rows(
                moved.astype(BF16), ref[:, side:]
            )

        copies[0].wait()
        first = shares(gate_all, w_gate_ref, slice(0, rows))
        second = shares(gate_all, w_gate_ref, slice(rows, lanes))
        copies[1].wait()
        mine_out[...] = (first + shares(up_all, w_up_ref, slice(0, rows))).astype(BF16)
        other_out[...] = (second + shares(up_all, w_up_ref, slice(rows, lanes))).astype(BF16)

    shapes = [(units, lanes)] * 3 + [(rows, width // 2)] * 2
    values = (pick, gate, up, hidden, gate_few, up_few)
    anywhere = pl.BlockSpec(memory_space=pl.ANY)
    return pl.pallas_call(
        kernel,
        in_specs=[whole_spec(value.shape) for value in values] + [anywhere] * 2,
        out_specs=[whole_spec(shape) for shape in shapes],
        out_shape=[jax.ShapeDtypeStruct(shape, BF16) for shape in shapes],
        scratch_shapes=weight_scratch(w_gate, 2),
    )(*values, w_gate, w_up)


def weight_gradients(mine, other, scale, gate, up, hidden, hidden_few, y_few):
    units = gate.shape[0]
    rows = mine.shape[0]
    few, width = y_few.shape
    block = 512

    def kernel(mine_ref, other_ref, scale_ref, gate_ref, up_ref, h_ref, hf_ref, y_ref, gate_out, up_out, down_out):
        first = (mine_ref[...].astype(F32) * scale_ref[:rows, :1]).astype(BF16)
        second = (other_ref[...].astype(F32) * scale_ref[rows:, :1]).astype(BF16)

        def both(ref):
            return matmul(ref[:, :rows], first) + matmul(ref[:, rows:], second)

        gate_out[...] = both(gate_ref).astype(BF16)
        up_out[...] = both(up_ref).astype(BF16)
        down_out[...] = (both(h_ref) + matmul(hf_ref[...], y_ref[...])).astype(BF16)

    across = lambda count: pl.BlockSpec((count, block), lambda i: (0, i))
    whole = lambda value: pl.BlockSpec(value.shape, lambda i: (0, 0))
    return pl.pallas_call(
        kernel,
        grid=(width // block,),
        in_specs=[across(rows), across(rows)]
        + [whole(value) for value in (scale, gate, up, hidden, hidden_few)]
        + [across(few)],
        out_specs=[across(units)] * 3,
        out_shape=[jax.ShapeDtypeStruct((units, width), BF16)] * 3,
    )(mine, other, scale, gate, up, hidden, hidden_few, y_few)


def on_device(saved_inputs, expert_ids, gate_weights, out_grad, gate_w, up_w, down_w):
    sections = lax.axis_size("section")
    devices = lax.axis_size("ep")
    chips = devices // 2
    section = lax.axis_index("section")
    place = lax.axis_index("ep")
    core = place % 2
    groups = [[2 * chip + k for chip in range(chips)] for k in range(2)]
    width = saved_inputs.shape[2]
    columns = width // devices
    slots = devices * CAP
    tokens = saved_inputs[0]
    token_count = tokens.shape[0]
    is_live = expert_ids[0] == 0
    w_gate = gate_w[0]
    w_up = up_w[0]
    w_down = down_w[0]

    live_count = jnp.sum(is_live.astype(jnp.int32), axis=1)
    pair_weight = jnp.sum(jnp.where(is_live, gate_weights[0], 0.0), axis=1)
    slot_index = jnp.cumsum(live_count) - live_count
    target = jnp.where(live_count == 1, slot_index, CAP)
    chosen = target[None, :] == jnp.arange(CAP, dtype=jnp.int32)[:, None]
    selector = chosen.astype(BF16)
    token_index = jnp.arange(token_count, dtype=jnp.int32)
    slot_token = jnp.sum(jnp.where(chosen, token_index[None, :] + 1, 0), axis=1) - 1
    slot_weight = jnp.sum(jnp.where(chosen, pair_weight[None, :], 0.0), axis=1)
    x_four = matmul(selector, tokens).astype(BF16)

    note = jnp.zeros((8, out_grad.shape[1]), BF16)
    note = lax.dynamic_update_slice(note, slot_token.astype(BF16)[None], (0, 0))
    parts = []
    remainder = slot_weight
    for _ in range(PARTS):
        part = lax.reduce_precision(remainder, 8, 7)
        parts.append(part.astype(BF16))
        remainder = remainder - part
    weight_parts = jnp.concatenate(parts)
    where = jnp.stack([section, core, place]).astype(jnp.int32)
    sent, x_four, slot_weight, selector, weight_parts, where = lax.optimization_barrier(
        (
            repeated(jnp.concatenate([out_grad, note], 0), sections),
            x_four,
            slot_weight,
            selector,
            weight_parts,
            where,
        )
    )
    above = exchange(sent, "section")
    upstream = above[:, :token_count]
    layer_tokens = above[:, token_count, :CAP].astype(jnp.int32)

    equal = layer_tokens[:, :, None, None] == layer_tokens[None, None]
    times = jnp.sum(equal.astype(jnp.int32), axis=(2, 3))
    times = jnp.where(layer_tokens >= 0, times, 0)
    code = jnp.where(times > 1, layer_tokens, -1).reshape(1, sections * CAP)

    up_four = lax.dot_general(
        selector, upstream, (((1,), (1,)), ((), ())), preferred_element_type=F32
    ).reshape(CAP, width)
    up_four = up_four.astype(BF16)
    extra = jnp.concatenate(
        [
            code.astype(BF16),
            weight_parts[None],
            jnp.max(times).astype(BF16).reshape(1, 1),
            jnp.zeros((1, LANES - (sections + PARTS) * CAP - 1), BF16),
        ],
        1,
    )
    extra = jnp.broadcast_to(extra, (ROWS, LANES))
    packed = jnp.concatenate([jnp.concatenate([x_four, up_four], 0), extra], 1)
    packed, above, layer_tokens = lax.optimization_barrier(
        (repeated(packed, chips), above, layer_tokens)
    )
    arrived = exchange(packed, "ep", groups)
    partner = from_partner(arrived, devices)
    mine = arrived.reshape(chips * ROWS, width + LANES)
    other = partner.reshape(chips * ROWS, width + LANES)

    (
        feeds_few,
        pick_few,
        weight_few,
        notes,
        scale,
        act,
        slope,
        hidden,
        gate_first,
        up_first,
        act_few,
        slope_few,
        hidden_few,
        gate_few,
        up_few,
        rows_few,
        y_few,
        share_few,
        counts,
    ) = first_pass(where, mine, other, w_gate, w_up, w_down, sections)
    chain_count = counts[0]
    trips = counts[1]
    layer_index = jnp.arange(sections, dtype=jnp.int32)

    def slow_plan(size):
        index = jnp.arange(size, dtype=jnp.int32)
        in_chain = (notes[:, : sections * CAP] >= 0).reshape(devices, sections, CAP)
        flags = jnp.swapaxes(in_chain, 0, 1).reshape(sections, slots)
        within = notes[:, : sections * CAP].astype(jnp.int32).reshape(devices, sections, CAP)
        base = token_count * jnp.arange(devices, dtype=jnp.int32)[:, None, None]
        token = jnp.swapaxes(within + base + 1, 0, 1).reshape(sections, slots)
        place = jnp.cumsum(flags.astype(jnp.int32), axis=1) - 1
        listed = flags[:, None, :] & (place[:, None, :] == index[None, :, None])
        tokens_of = jnp.sum(jnp.where(listed, token[:, None, :], 0), axis=2)
        own_token = lax.dynamic_index_in_dim(tokens_of, section, 0, keepdims=False)
        own = lax.dynamic_index_in_dim(listed, section, 0, keepdims=False)
        parts = notes[:, sections * CAP : (sections + PARTS) * CAP].reshape(devices, PARTS, CAP)
        weight = jnp.sum(jnp.where(own, jnp.sum(parts, axis=1).reshape(1, slots), 0.0), axis=1)
        feeds = (
            (own_token[:, None, None] == tokens_of[None])
            & (own_token[:, None, None] > 0)
            & (layer_index[None, :, None] > section)
        )
        halves = own.reshape(size, 2, chips, CAP)
        halves = jnp.where(core == 0, halves, halves[:, ::-1])
        halves = jnp.concatenate([halves, jnp.zeros_like(halves)], 3)
        return (
            feeds.reshape(size, sections * size).astype(BF16),
            halves.reshape(size, devices * ROWS).astype(BF16),
            jnp.broadcast_to(weight[:, None], (size, LANES)),
        )

    def slow_start(size):
        feeds, pick, weight = slow_plan(size)
        half = chips * ROWS
        y_pick = jnp.roll(pick, CAP, axis=1)
        exact = lambda value: lax.dot_general(
            value,
            pick.astype(F32),
            (((1,), (1,)), ((), ())),
            precision=lax.Precision.HIGHEST,
        )
        cut = lambda value: lax.dynamic_slice(value, (0, place * columns), (half, columns))
        gate = project(gate_first, pick).astype(BF16)
        up = project(up_first, pick).astype(BF16)
        share = (sum_rows(gate, w_gate) + sum_rows(up, w_up)).astype(BF16)
        return (
            feeds,
            pick,
            weight,
            exact(act),
            exact(slope),
            project(hidden, pick).astype(BF16),
            gate,
            up,
            matmul(y_pick[:, :half], cut(mine)) + matmul(y_pick[:, half:], cut(other)),
            jnp.zeros((size, width), BF16),
            jnp.swapaxes(share.reshape(size, devices, columns), 0, 1),
        )

    def finish(size):
        if size == FEW:
            start = (
                feeds_few,
                pick_few,
                weight_few,
                act_few,
                slope_few,
                hidden_few,
                gate_few,
                up_few,
                rows_few,
                y_few,
                share_few,
            )
        else:
            start = slow_start(size)
        feeds, pick, weight, act_rows, slope_rows, hidden_rows = start[:6]
        first_rows = start[8]

        def more(state):
            return state[0] < trips

        def step(state):
            share, trip = lax.optimization_barrier((state[4], state[0] + 1))
            summed = jnp.sum(exchange(share, "ep").astype(F32), axis=0).astype(BF16)
            layers = exchange(repeated(summed, sections), "section")
            above_rows = first_rows + matmul(feeds, layers.reshape(sections * size, columns))
            above_rows = lax.reduce_precision(above_rows, 8, 7)
            y_part = (weight * above_rows).astype(BF16)
            blocks = exchange(repeated(y_part, devices), "ep")
            y, gate, up, share = chain_step(blocks, act_rows, slope_rows, w_gate, w_up, w_down)
            return (trip, y, gate, up, share)

        state = (jnp.int32(0), start[9], start[6], start[7], start[10])
        _, y, gate, up, _ = lax.while_loop(more, step, state)
        gate, up, hidden_kept, share_mine, share_other = merge_chains(
            pick, gate_first, up_first, hidden, gate, up, w_gate, w_up
        )

        theirs = from_partner(share_other, devices)
        chip_sum = (share_mine.astype(F32) + theirs.astype(F32)).astype(BF16)
        tiles = exchange(chip_sum.reshape(chips, ROWS, width // 2), "ep", groups)
        back = jnp.sum(tiles.astype(F32), axis=0).astype(BF16)
        all_back = exchange(repeated(back, sections), "section")
        all_back = all_back.reshape(sections, 2, CAP, width // 2)
        all_back = jnp.swapaxes(all_back, 1, 2).reshape(sections * CAP, width)
        takes = (layer_tokens[:, :, None] == token_index[None, None, :]) & (
            layer_index[:, None, None] >= section
        )
        takes = takes.reshape(sections * CAP, token_count).astype(BF16)
        whole = jnp.swapaxes(above[:, :token_count], 0, 1).reshape(token_count, width)
        result = whole.astype(F32) + sum_rows(takes, all_back)
        grads = weight_gradients(mine, other, scale, gate, up, hidden_kept, hidden_rows, y)
        return (result.astype(BF16), *grads)

    outputs = lax.cond(chain_count <= FEW, lambda: finish(FEW), lambda: finish(slots))
    return tuple(output[None] for output in outputs)


def solution(mesh):
    by_rows = P("section", "ep", None)
    return jax.shard_map(
        on_device,
        mesh=mesh,
        in_specs=(by_rows, by_rows, by_rows, P("ep", "section"), by_rows, by_rows, by_rows),
        out_specs=(by_rows, by_rows, by_rows, by_rows),
        check_vma=False,
    )
```

```python
import jax
import jax.numpy as jnp
from jax import lax
from jax.experimental import pallas as pl
from jax.experimental.pallas import tpu as pltpu
from jax.sharding import PartitionSpec as P

CAP = 4
ROWS = 2 * CAP
FEW = 16
PARTS = 3
LANES = 128
F32 = jnp.float32
BF16 = jnp.bfloat16


def exchange(blocks, axis, groups=None):
    return lax.all_to_all(blocks, axis, 0, 0, tiled=True, axis_index_groups=groups)


def repeated(value, count):
    return jnp.broadcast_to(value[None], (count, *value.shape))


def from_partner(value, devices):
    return lax.ppermute(value, "ep", [(i, i ^ 1) for i in range(devices)])


def project(row_data, weight):
    return lax.dot_general(
        row_data, weight, (((1,), (1,)), ((), ())), preferred_element_type=F32
    )


def matmul(left, right):
    return jnp.dot(left, right, preferred_element_type=F32)


def sum_rows(left, right):
    return lax.dot_general(
        left, right, (((0,), (0,)), ((), ())), preferred_element_type=F32
    )


def iota(shape, dim):
    return lax.broadcasted_iota(jnp.int32, shape, dim)


def grant(mebibytes):
    return pltpu.CompilerParams(vmem_limit_bytes=mebibytes << 20)


def as_float(mask):
    return jnp.where(mask, 1.0, 0.0)


def whole_spec(shape):
    return pl.BlockSpec(shape, lambda: (0,) * len(shape))


def first_pass(where, mine, other, w_gate, w_up, w_down, sections):
    half = mine.shape[0] // ROWS
    rows = half * ROWS
    devices = 2 * half
    codes = sections * CAP
    ending = codes + PARTS * CAP
    units, width = w_gate.shape
    columns = width // devices

    def kernel(
        where_ref,
        mine_ref,
        other_ref,
        w_gate_ref,
        w_up_ref,
        w_down_ref,
        feeds_ref,
        pick_ref,
        weight_ref,
        note_ref,
        column_ref,
        scaled_ref,
        act_ref,
        slope_ref,
        hidden_ref,
        gate_ref,
        up_ref,
        act_few_ref,
        slope_few_ref,
        hidden_few_ref,
        gate_few_ref,
        up_few_ref,
        rows_few_ref,
        y_few_ref,
        share_ref,
        count_ref,
    ):
        section = where_ref[0]
        core = where_ref[1]
        place = where_ref[2]

        lead = as_float(iota((half, rows), 1) == ROWS * iota((half, rows), 0)).astype(BF16)
        tiles = [ref[:, width:] for ref in (mine_ref, other_ref)]
        near = matmul(lead, tiles[0])
        far = matmul(lead, tiles[1])
        note = jnp.concatenate([jnp.where(core == 0, near, far), jnp.where(core == 0, far, near)], 0)
        note_ref[...] = note
        lane = iota((devices, LANES), 1)
        code = jnp.where(lane < codes, note, -1.0)
        flag = as_float(code >= 0)
        row = iota((LANES, LANES), 0)
        col = iota((LANES, LANES), 1)
        same_layer = row // CAP == col // CAP
        per_layer = matmul(flag, as_float(same_layer))
        count_ref[0] = jnp.max(jnp.sum(per_layer, axis=0, keepdims=True)).astype(jnp.int32)
        most = jnp.max(jnp.where(lane == codes + PARTS * CAP, note, 0.0))
        count_ref[1] = most.astype(jnp.int32) - 1
        before = as_float(iota((devices, devices), 1) < iota((devices, devices), 0))
        rank = matmul(before, per_layer) + matmul(flag, as_float(same_layer & (row < col)))
        rank = (rank + 1.0) * flag
        token = (code + 1.0) * flag
        owned = as_float(iota((8, LANES), 1) == iota((8, LANES), 0) + CAP * section)
        own_rank = project(owned, rank)
        own_token = project(owned, token)
        entry = iota((FEW, devices), 0).astype(F32) + 1.0
        device = iota((devices, 2 * rows), 0)
        spot = iota((devices, 2 * rows), 1)
        home = rows * ((device // half + core) % 2) + ROWS * (device % half)
        held = jnp.zeros((FEW, 1), F32)
        weight = jnp.zeros((FEW, LANES), F32)
        groups = jnp.zeros((FEW, devices), F32)
        pick = jnp.zeros((FEW, 2 * rows), F32)
        few_lane = iota((FEW, LANES), 1)
        for slot in range(CAP):
            here = as_float(own_rank[slot : slot + 1] == entry)
            groups = groups + here
            held = held + jnp.sum(here * own_token[slot : slot + 1], axis=1, keepdims=True)
            part = matmul(here, note)
            wanted = (few_lane >= codes) & (few_lane < ending) & (few_lane % CAP == slot)
            weight = weight + jnp.where(wanted, part, 0.0)
            pick = pick + matmul(here, as_float(spot == home + slot))
        near_rank = matmul(groups, rank)
        near_token = matmul(groups, token)
        match = (near_token == held) & (near_token > 0) & (few_lane // CAP > section)
        source = jnp.where(match & (few_lane < codes), near_rank, 0.0)
        feeds = jnp.zeros((FEW, LANES), F32)
        for slot in range(CAP):
            spread = as_float((row // CAP == col // FEW) & (row % CAP == slot))
            feeds = feeds + as_float(
                matmul(source, spread) == (few_lane % FEW + 1).astype(F32)
            )
        feeds_ref[...] = feeds.astype(BF16)
        pick_low = pick.astype(BF16)
        pick_ref[...] = pick_low
        weight_ref[...] = jnp.broadcast_to(
            jnp.sum(weight, axis=1, keepdims=True), (FEW, LANES)
        )

        kind = iota((rows, LANES), 0) % ROWS - CAP
        tile_lane = iota((rows, LANES), 1)
        wanted = (tile_lane >= codes) & (tile_lane < ending) & (tile_lane % CAP == kind)
        halves = []
        for index, ref in enumerate((mine_ref, other_ref)):
            scale = jnp.sum(
                jnp.where(wanted, tiles[index].astype(F32), 0.0), axis=1, keepdims=True
            )
            scale = jnp.where(kind[:, :1] >= 0, scale, 1.0)
            halves.append((ref[:, :width].astype(F32) * scale).astype(BF16))
            scaled_ref[index * rows : (index + 1) * rows, :] = halves[index]
        y_pick = pltpu.roll(pick, CAP, 1).astype(BF16)
        y_few_ref[...] = (
            matmul(y_pick[:, :rows], halves[0]) + matmul(y_pick[:, rows:], halves[1])
        ).astype(BF16)
        spot = pl.ds(pl.multiple_of(place * columns, columns), columns)
        column_ref[:rows, :] = mine_ref[:, spot]
        column_ref[rows:, :] = other_ref[:, spot]
        rows_few_ref[...] = matmul(y_pick, column_ref[...])
        x_lane = iota((units, 2 * rows), 1) % ROWS < CAP
        grad = pltpu.roll(project(w_down_ref[...], scaled_ref[...]), 2 * rows - CAP, 1)
        gate_pre = project(w_gate_ref[...], scaled_ref[...])
        up_pre = project(w_up_ref[...], scaled_ref[...])
        sig = 1.0 / (1.0 + jnp.exp(-gate_pre))
        act = jnp.where(x_lane, gate_pre * sig, 0.0)
        slope = jnp.where(x_lane, up_pre * sig * (1.0 + gate_pre * (1.0 - sig)), 0.0)
        act_ref[...] = act
        slope_ref[...] = slope
        hidden_ref[...] = (act * up_pre).astype(BF16)
        gate_ref[...] = (grad * slope).astype(BF16)
        up_ref[...] = (grad * act).astype(BF16)

        def exact(value):
            return lax.dot_general(
                value,
                pick,
                (((1,), (1,)), ((), ())),
                precision=lax.Precision.HIGHEST,
                preferred_element_type=F32,
            )

        act_few_ref[...] = exact(act_ref[...])
        slope_few_ref[...] = exact(slope_ref[...])
        hidden_few_ref[...] = project(hidden_ref[...], pick_low).astype(BF16)
        gate_few = project(gate_ref[...], pick_low).astype(BF16)
        up_few = project(up_ref[...], pick_low).astype(BF16)
        gate_few_ref[...] = gate_few
        up_few_ref[...] = up_few
        share = (sum_rows(gate_few, w_gate_ref[...]) + sum_rows(up_few, w_up_ref[...])).astype(BF16)
        for index in range(devices):
            share_ref[index] = share[:, index * columns : (index + 1) * columns]

    shapes = [
        ((FEW, sections * FEW), BF16),
        ((FEW, ROWS * devices), BF16),
        ((FEW, LANES), F32),
        ((devices, LANES), F32),
        ((2 * rows, columns), BF16),
        ((2 * rows, width), BF16),
        ((units, 2 * rows), F32),
        ((units, 2 * rows), F32),
        ((units, 2 * rows), BF16),
        ((units, 2 * rows), BF16),
        ((units, 2 * rows), BF16),
        ((units, FEW), F32),
        ((units, FEW), F32),
        ((units, FEW), BF16),
        ((units, FEW), BF16),
        ((units, FEW), BF16),
        ((FEW, columns), F32),
        ((FEW, width), BF16),
        ((devices, FEW, columns), BF16),
    ]
    smem = pl.BlockSpec(memory_space=pltpu.SMEM)
    return pl.pallas_call(
        kernel,
        compiler_params=grant(28),
        in_specs=[smem, whole_spec(mine.shape), whole_spec(other.shape)] + [whole_spec(w_gate.shape)] * 3,
        out_specs=[whole_spec(shape) for shape, _ in shapes] + [smem],
        out_shape=[jax.ShapeDtypeStruct(shape, dtype) for shape, dtype in shapes]
        + [jax.ShapeDtypeStruct((2,), jnp.int32)],
    )(where, mine, other, w_gate, w_up, w_down)


def chain_step(y_blocks, act_few, slope_few, w_gate, w_up, w_down):
    devices, size, columns = y_blocks.shape
    units, width = w_gate.shape

    def kernel(
        blocks_ref,
        act_ref,
        slope_ref,
        w_gate_ref,
        w_up_ref,
        w_down_ref,
        y_ref,
        gate_few_ref,
        up_few_ref,
        share_ref,
    ):
        for index in range(devices):
            y_ref[:, index * columns : (index + 1) * columns] = blocks_ref[index]
        grad = project(w_down_ref[...], y_ref[...])
        gate_few = (grad * slope_ref[...]).astype(BF16)
        up_few = (grad * act_ref[...]).astype(BF16)
        gate_few_ref[...] = gate_few
        up_few_ref[...] = up_few
        share = sum_rows(gate_few, w_gate_ref[...])
        share = (share + sum_rows(up_few, w_up_ref[...])).astype(BF16)
        for index in range(devices):
            share_ref[index] = share[:, index * columns : (index + 1) * columns]

    shapes = [(size, width), (units, size), (units, size), (devices, size, columns)]
    return pl.pallas_call(
        kernel,
        compiler_params=grant(16),
        in_specs=[whole_spec(value.shape) for value in (y_blocks, act_few, slope_few)]
        + [whole_spec(w_gate.shape)] * 3,
        out_specs=[whole_spec(shape) for shape in shapes],
        out_shape=[jax.ShapeDtypeStruct(shape, BF16) for shape in shapes],
    )(y_blocks, act_few, slope_few, w_gate, w_up, w_down)


def merge_chains(pick, gate, up, hidden, gate_few, up_few, w_gate, w_up):
    units, width = w_gate.shape
    lanes = gate.shape[1]
    rows = lanes // 2

    def kernel(
        pick_ref,
        gate_ref,
        up_ref,
        hidden_ref,
        gate_few_ref,
        up_few_ref,
        w_gate_ref,
        w_up_ref,
        gate_out,
        up_out,
        hidden_out,
        mine_out,
        other_out,
    ):
        pick_low = pick_ref[...]
        keep = jnp.sum(pick_low.astype(F32), axis=0, keepdims=True) == 0.0
        gate_all = jnp.where(keep, gate_ref[...].astype(F32), matmul(gate_few_ref[...], pick_low))
        up_all = jnp.where(keep, up_ref[...].astype(F32), matmul(up_few_ref[...], pick_low))
        gate_out[...] = gate_all.astype(BF16)
        up_out[...] = up_all.astype(BF16)
        kept = jnp.where(keep, hidden_ref[...].astype(F32), 0.0)
        hidden_out[...] = pltpu.roll(kept, CAP, 1).astype(BF16)
        side = width // 2

        def shares(value, ref):
            moved = pltpu.roll(value, CAP, 1)
            return sum_rows(value.astype(BF16), ref[:, :side]) + sum_rows(
                moved.astype(BF16), ref[:, side:]
            )

        share = (shares(gate_all, w_gate_ref) + shares(up_all, w_up_ref)).astype(BF16)
        mine_out[...] = share[:rows]
        other_out[...] = share[rows:]

    shapes = [(units, lanes)] * 3 + [(rows, width // 2)] * 2
    values = (pick, gate, up, hidden, gate_few, up_few)
    return pl.pallas_call(
        kernel,
        compiler_params=grant(16),
        in_specs=[whole_spec(value.shape) for value in values] + [whole_spec(w_gate.shape)] * 2,
        out_specs=[whole_spec(shape) for shape in shapes],
        out_shape=[jax.ShapeDtypeStruct(shape, BF16) for shape in shapes],
    )(*values, w_gate, w_up)


def weight_gradients(scaled, gate, up, hidden, hidden_few, y_few):
    units, rows = gate.shape
    few, width = y_few.shape
    block = 512

    def kernel(rows_ref, gate_ref, up_ref, h_ref, hf_ref, y_ref, gate_out, up_out, down_out):
        gate_out[...] = matmul(gate_ref[...], rows_ref[...]).astype(BF16)
        up_out[...] = matmul(up_ref[...], rows_ref[...]).astype(BF16)
        down_out[...] = (
            matmul(h_ref[...], rows_ref[...]) + matmul(hf_ref[...], y_ref[...])
        ).astype(BF16)

    across = lambda count: pl.BlockSpec((count, block), lambda i: (0, i))
    whole = lambda value: pl.BlockSpec(value.shape, lambda i: (0, 0))
    return pl.pallas_call(
        kernel,
        compiler_params=grant(16),
        grid=(width // block,),
        in_specs=[across(rows)]
        + [whole(value) for value in (gate, up, hidden, hidden_few)]
        + [across(few)],
        out_specs=[across(units)] * 3,
        out_shape=[jax.ShapeDtypeStruct((units, width), BF16)] * 3,
    )(scaled, gate, up, hidden, hidden_few, y_few)


def prepare(ids, weights, tokens, out_grad, sections):
    count, width = tokens.shape
    part_width = out_grad.shape[1]
    codes = sections * CAP

    def kernel(ids_ref, weights_ref, tokens_ref, grad_ref, sent_ref, x_ref, select_ref, weight_ref):
        live = as_float(ids_ref[...] == 0)
        weight = jnp.sum(live * weights_ref[...], axis=0, keepdims=True)
        live = jnp.sum(live, axis=0, keepdims=True)
        row = iota((count, count), 0)
        col = iota((count, count), 1)
        slot = matmul(jnp.broadcast_to(live, (8, count)), as_float(row < col))[:1]
        slot = jnp.where(live > 0, slot, -1.0)
        at_slot = as_float(slot == row.astype(F32))
        index = iota((8, count), 1).astype(F32) + 1.0
        token = project(index, at_slot) - 1.0
        tile = jnp.concatenate([token, jnp.zeros((8, part_width - count), F32)], 1).astype(BF16)
        for layer in range(sections):
            sent_ref[layer, :count, :] = grad_ref[...]
            sent_ref[layer, count:, :] = tile
        select = at_slot[:8].astype(BF16)
        select_ref[...] = select
        x_ref[...] = matmul(select, tokens_ref[...]).astype(BF16)
        parts = jnp.zeros((8, LANES), F32)
        remainder = weight
        for part in range(PARTS):
            piece = remainder.astype(BF16).astype(F32)
            remainder = remainder - piece
            moved = as_float((slot + (codes + part * CAP) == row.astype(F32)) & (slot >= 0))
            parts = parts + project(jnp.broadcast_to(piece, (8, count)), moved)
        weight_ref[...] = parts

    shapes = [
        ((sections, count + 8, part_width), BF16),
        ((8, width), BF16),
        ((8, count), BF16),
        ((8, LANES), F32),
    ]
    return pl.pallas_call(
        kernel,
        compiler_params=grant(8),
        in_specs=[whole_spec(value.shape) for value in (ids, weights, tokens, out_grad)],
        out_specs=[whole_spec(shape) for shape, _ in shapes],
        out_shape=[jax.ShapeDtypeStruct(shape, dtype) for shape, dtype in shapes],
    )(ids, weights, tokens, out_grad)


def pack(above, x_four, select, weight, chips):
    sections, tall, part_width = above.shape
    count = tall - 8
    width = x_four.shape[1]
    codes = sections * CAP

    def kernel(above_ref, x_ref, select_ref, weight_ref, packed_ref, token_ref):
        tokens = jnp.concatenate(
            [above_ref[layer, count:, :LANES].astype(F32)[:1] for layer in range(sections)], 0
        )
        row = iota((LANES, LANES), 0)
        col = iota((LANES, LANES), 1)
        spread = matmul(tokens, as_float((row < CAP) & (col % CAP == row)))
        lane = iota((sections, LANES), 1)
        layer = iota((sections, LANES), 0)
        pick_lane = lambda size: jnp.sum(
            jnp.where(lane // size == layer, spread, 0.0), axis=0, keepdims=True
        )
        flat = pick_lane(CAP)
        lane = lane[:1]
        flat = jnp.where(lane < codes, flat, -1.0)
        times = jnp.zeros((1, LANES), F32)
        for slot in range(CAP):
            times = times + jnp.sum(
                as_float(tokens[:, slot : slot + 1] == flat), axis=0, keepdims=True
            )
        times = jnp.where(flat >= 0, times, 0.0)
        code = jnp.where(times > 1, flat, -1.0)
        most = jnp.max(times)
        note = jnp.where(lane < codes, code, weight_ref[:1])
        note = jnp.where(lane == codes + PARTS * CAP, most, note)
        note = jnp.broadcast_to(note, (ROWS, LANES)).astype(BF16)
        lane = iota((sections, LANES), 1)
        token_ref[...] = jnp.broadcast_to(pick_lane(2 * CAP), (8, LANES))
        lower = pltpu.roll(select_ref[...].astype(F32), CAP, 0).astype(BF16)
        pieces = [
            (matmul(lower, above_ref[part, :count, :]) + x_ref[:, part * part_width : (part + 1) * part_width].astype(F32)).astype(BF16)
            for part in range(sections)
        ]
        for chip in range(chips):
            for part in range(sections):
                packed_ref[chip, :, part * part_width : (part + 1) * part_width] = pieces[part]
            packed_ref[chip, :, width:] = note

    shapes = [((chips, ROWS, width + LANES), BF16), ((8, LANES), F32)]
    return pl.pallas_call(
        kernel,
        compiler_params=grant(8),
        in_specs=[whole_spec(value.shape) for value in (above, x_four, select, weight)],
        out_specs=[whole_spec(shape) for shape, _ in shapes],
        out_shape=[jax.ShapeDtypeStruct(shape, dtype) for shape, dtype in shapes],
    )(above, x_four, select, weight)


def assemble(where, tokens, above, back):
    sections, tall, part_width = above.shape
    count = tall - 8
    rows, side = back.shape
    per_side = side // part_width

    def kernel(where_ref, token_ref, above_ref, back_ref, out_ref):
        step = pl.program_id(0)
        lane = iota((count, rows), 1)
        taken = (
            (token_ref[:1, :rows] == iota((count, rows), 0).astype(F32))
            & (lane // (2 * CAP) >= where_ref[0])
            & (lane // CAP % 2 == step // per_side)
        )
        added = matmul(as_float(taken).astype(BF16), back_ref[...])
        out_ref[...] = (above_ref[0, :count, :].astype(F32) + added).astype(BF16)

    return pl.pallas_call(
        kernel,
        compiler_params=grant(8),
        grid=(sections,),
        in_specs=[
            pl.BlockSpec(memory_space=pltpu.SMEM),
            pl.BlockSpec(tokens.shape, lambda i: (0, 0)),
            pl.BlockSpec((1, tall, part_width), lambda i: (i, 0, 0)),
            pl.BlockSpec((rows, part_width), lambda i: (0, i % per_side)),
        ],
        out_specs=pl.BlockSpec((count, part_width), lambda i: (0, i)),
        out_shape=jax.ShapeDtypeStruct((count, 2 * side), BF16),
    )(where, tokens, above, back)


def on_device(saved_inputs, expert_ids, gate_weights, out_grad, gate_w, up_w, down_w):
    sections = lax.axis_size("section")
    devices = lax.axis_size("ep")
    chips = devices // 2
    section = lax.axis_index("section")
    place = lax.axis_index("ep")
    core = place % 2
    groups = [[2 * chip + k for chip in range(chips)] for k in range(2)]
    width = saved_inputs.shape[2]
    columns = width // devices
    slots = devices * CAP
    tokens = saved_inputs[0]
    token_count = tokens.shape[0]
    w_gate = gate_w[0]
    w_up = up_w[0]
    w_down = down_w[0]

    where = jnp.stack([section, core, place]).astype(jnp.int32)
    sent, x_four, select, slot_weight = prepare(
        expert_ids[0].T, gate_weights[0].T, tokens, out_grad, sections
    )
    sent, where = lax.optimization_barrier((sent, where))
    above = exchange(sent, "section")
    packed, all_tokens = pack(above, x_four, select, slot_weight, chips)
    arrived = exchange(packed, "ep", groups)
    partner = from_partner(arrived, devices)
    mine = arrived.reshape(chips * ROWS, width + LANES)
    other = partner.reshape(chips * ROWS, width + LANES)

    (
        feeds_few,
        pick_few,
        weight_few,
        notes,
        column,
        scaled,
        act,
        slope,
        hidden,
        gate_first,
        up_first,
        act_few,
        slope_few,
        hidden_few,
        gate_few,
        up_few,
        rows_few,
        y_few,
        share_few,
        counts,
    ) = first_pass(where, mine, other, w_gate, w_up, w_down, sections)
    chain_count = counts[0]
    trips = counts[1]
    def slow_plan(size):
        layer_index = jnp.arange(sections, dtype=jnp.int32)
        index = jnp.arange(size, dtype=jnp.int32)
        in_chain = (notes[:, : sections * CAP] >= 0).reshape(devices, sections, CAP)
        flags = jnp.swapaxes(in_chain, 0, 1).reshape(sections, slots)
        within = notes[:, : sections * CAP].astype(jnp.int32).reshape(devices, sections, CAP)
        base = token_count * jnp.arange(devices, dtype=jnp.int32)[:, None, None]
        token = jnp.swapaxes(within + base + 1, 0, 1).reshape(sections, slots)
        place = jnp.cumsum(flags.astype(jnp.int32), axis=1) - 1
        listed = flags[:, None, :] & (place[:, None, :] == index[None, :, None])
        tokens_of = jnp.sum(jnp.where(listed, token[:, None, :], 0), axis=2)
        own_token = lax.dynamic_index_in_dim(tokens_of, section, 0, keepdims=False)
        own = lax.dynamic_index_in_dim(listed, section, 0, keepdims=False)
        parts = notes[:, sections * CAP : (sections + PARTS) * CAP].reshape(devices, PARTS, CAP)
        weight = jnp.sum(jnp.where(own, jnp.sum(parts, axis=1).reshape(1, slots), 0.0), axis=1)
        feeds = (
            (own_token[:, None, None] == tokens_of[None])
            & (own_token[:, None, None] > 0)
            & (layer_index[None, :, None] > section)
        )
        halves = own.reshape(size, 2, chips, CAP)
        halves = jnp.where(core == 0, halves, halves[:, ::-1])
        halves = jnp.concatenate([halves, jnp.zeros_like(halves)], 3)
        return (
            feeds.reshape(size, sections * size).astype(BF16),
            halves.reshape(size, devices * ROWS).astype(BF16),
            jnp.broadcast_to(weight[:, None], (size, LANES)),
        )

    def slow_start(size):
        feeds, pick, weight = slow_plan(size)
        exact = lambda value: lax.dot_general(
            value,
            pick.astype(F32),
            (((1,), (1,)), ((), ())),
            precision=lax.Precision.HIGHEST,
        )
        gate = project(gate_first, pick).astype(BF16)
        up = project(up_first, pick).astype(BF16)
        share = (sum_rows(gate, w_gate) + sum_rows(up, w_up)).astype(BF16)
        return (
            feeds,
            pick,
            weight,
            exact(act),
            exact(slope),
            project(hidden, pick).astype(BF16),
            gate,
            up,
            matmul(jnp.roll(pick, CAP, axis=1), column),
            jnp.zeros((size, width), BF16),
            jnp.swapaxes(share.reshape(size, devices, columns), 0, 1),
        )

    def finish(size):
        if size == FEW:
            start = (
                feeds_few,
                pick_few,
                weight_few,
                act_few,
                slope_few,
                hidden_few,
                gate_few,
                up_few,
                rows_few,
                y_few,
                share_few,
            )
        else:
            start = slow_start(size)
        feeds, pick, weight, act_rows, slope_rows, hidden_rows = start[:6]
        first_rows = start[8]

        def more(state):
            return state[0] < trips

        def step(state):
            share, trip = lax.optimization_barrier((state[4], state[0] + 1))
            summed = jnp.sum(exchange(share, "ep").astype(F32), axis=0)
            summed = lax.reduce_precision(summed, 8, 7).astype(BF16)
            layers = exchange(repeated(summed, sections), "section")
            above_rows = first_rows + matmul(feeds, layers.reshape(sections * size, columns))
            above_rows = lax.reduce_precision(above_rows, 8, 7)
            y_part = (weight * above_rows).astype(BF16)
            blocks = exchange(repeated(y_part, devices), "ep")
            y, gate, up, share = chain_step(blocks, act_rows, slope_rows, w_gate, w_up, w_down)
            return (trip, y, gate, up, share)

        state = (jnp.int32(0), start[9], start[6], start[7], start[10])
        _, y, gate, up, _ = lax.while_loop(more, step, state)
        gate, up, hidden_kept, share_mine, share_other = merge_chains(
            pick, gate_first, up_first, hidden, gate, up, w_gate, w_up
        )

        theirs = from_partner(share_other, devices)
        chip_sum = (share_mine.astype(F32) + theirs.astype(F32)).astype(BF16)
        tiles = exchange(chip_sum.reshape(chips, ROWS, width // 2), "ep", groups)
        back = lax.reduce_precision(jnp.sum(tiles.astype(F32), axis=0), 8, 7).astype(BF16)
        all_back = exchange(repeated(back, sections), "section")
        grads = weight_gradients(scaled, gate, up, hidden_kept, hidden_rows, y)
        result = assemble(where, all_tokens, above, all_back.reshape(sections * ROWS, width // 2))
        return (result, *grads)

    outputs = lax.cond(chain_count <= FEW, lambda: finish(FEW), lambda: finish(slots))
    return tuple(output[None] for output in outputs)


def solution(mesh):
    by_rows = P("section", "ep", None)
    return jax.shard_map(
        on_device,
        mesh=mesh,
        in_specs=(by_rows, by_rows, by_rows, P("ep", "section"), by_rows, by_rows, by_rows),
        out_specs=(by_rows, by_rows, by_rows, by_rows),
        check_vma=False,
    )
```

```python
import jax
import jax.numpy as jnp
from jax import lax
from jax.experimental import pallas as pl
from jax.experimental.pallas import tpu as pltpu
from jax.sharding import PartitionSpec as P

CAP = 4
ROWS = 2 * CAP
FEW = 16
PARTS = 3
LANES = 128
F32 = jnp.float32
BF16 = jnp.bfloat16


def exchange(blocks, axis, groups=None):
    return lax.all_to_all(blocks, axis, 0, 0, tiled=True, axis_index_groups=groups)


def repeated(value, count):
    return jnp.broadcast_to(value[None], (count, *value.shape))


def from_partner(value, devices):
    return lax.ppermute(value, "ep", [(i, i ^ 1) for i in range(devices)])


def project(row_data, weight):
    return lax.dot_general(
        row_data, weight, (((1,), (1,)), ((), ())), preferred_element_type=F32
    )


def matmul(left, right):
    return jnp.dot(left, right, preferred_element_type=F32)


def sum_rows(left, right):
    return lax.dot_general(
        left, right, (((0,), (0,)), ((), ())), preferred_element_type=F32
    )


def iota(shape, dim):
    return lax.broadcasted_iota(jnp.int32, shape, dim)


def grant(mebibytes):
    return pltpu.CompilerParams(vmem_limit_bytes=mebibytes << 20)


def as_float(mask):
    return jnp.where(mask, 1.0, 0.0)


def whole_spec(shape):
    return pl.BlockSpec(shape, lambda: (0,) * len(shape))


def first_pass(where, x_mine, x_other, mine, other, w_gate, w_up, w_down, sections):
    half = mine.shape[0] // ROWS
    rows = half * ROWS
    side = x_mine.shape[1]
    devices = 2 * half
    codes = sections * CAP
    ending = codes + PARTS * CAP
    units, width = w_gate.shape
    columns = width // devices

    def kernel(
        where_ref,
        x_mine_ref,
        x_other_ref,
        mine_ref,
        other_ref,
        w_gate_ref,
        w_up_ref,
        w_down_ref,
        feeds_ref,
        pick_ref,
        weight_ref,
        note_ref,
        column_ref,
        rows_ref,
        scaled_ref,
        act_ref,
        slope_ref,
        hidden_ref,
        gate_ref,
        up_ref,
        act_few_ref,
        slope_few_ref,
        hidden_few_ref,
        gate_few_ref,
        up_few_ref,
        rows_few_ref,
        y_few_ref,
        share_ref,
        count_ref,
    ):
        section = where_ref[0]
        core = where_ref[1]
        place = where_ref[2]

        lead = as_float(iota((half, rows), 1) == ROWS * iota((half, rows), 0)).astype(BF16)
        tiles = [ref[:, side:] for ref in (mine_ref, other_ref)]
        near = matmul(lead, tiles[0])
        far = matmul(lead, tiles[1])
        note = jnp.concatenate([jnp.where(core == 0, near, far), jnp.where(core == 0, far, near)], 0)
        note_ref[...] = note
        lane = iota((devices, LANES), 1)
        code = jnp.where(lane < codes, note, -1.0)
        flag = as_float(code >= 0)
        row = iota((LANES, LANES), 0)
        col = iota((LANES, LANES), 1)
        same_layer = row // CAP == col // CAP
        per_layer = matmul(flag, as_float(same_layer))
        count_ref[0] = jnp.max(jnp.sum(per_layer, axis=0, keepdims=True)).astype(jnp.int32)
        most = jnp.max(jnp.where(lane == codes + PARTS * CAP, note, 0.0))
        count_ref[1] = most.astype(jnp.int32) - 1
        before = as_float(iota((devices, devices), 1) < iota((devices, devices), 0))
        rank = matmul(before, per_layer) + matmul(flag, as_float(same_layer & (row < col)))
        rank = (rank + 1.0) * flag
        token = (code + 1.0) * flag
        owned = as_float(iota((8, LANES), 1) == iota((8, LANES), 0) + CAP * section)
        own_rank = project(owned, rank)
        own_token = project(owned, token)
        entry = iota((FEW, devices), 0).astype(F32) + 1.0
        device = iota((devices, 2 * rows), 0)
        spot = iota((devices, 2 * rows), 1)
        home = rows * ((device // half + core) % 2) + ROWS * (device % half)
        held = jnp.zeros((FEW, 1), F32)
        weight = jnp.zeros((FEW, LANES), F32)
        groups = jnp.zeros((FEW, devices), F32)
        pick = jnp.zeros((FEW, 2 * rows), F32)
        few_lane = iota((FEW, LANES), 1)
        for slot in range(CAP):
            here = as_float(own_rank[slot : slot + 1] == entry)
            groups = groups + here
            held = held + jnp.sum(here * own_token[slot : slot + 1], axis=1, keepdims=True)
            part = matmul(here, note)
            wanted = (few_lane >= codes) & (few_lane < ending) & (few_lane % CAP == slot)
            weight = weight + jnp.where(wanted, part, 0.0)
            pick = pick + matmul(here, as_float(spot == home + slot))
        near_rank = matmul(groups, rank)
        near_token = matmul(groups, token)
        match = (near_token == held) & (near_token > 0) & (few_lane // CAP > section)
        source = jnp.where(match & (few_lane < codes), near_rank, 0.0)
        feeds = jnp.zeros((FEW, LANES), F32)
        for slot in range(CAP):
            spread = as_float((row // CAP == col // FEW) & (row % CAP == slot))
            feeds = feeds + as_float(
                matmul(source, spread) == (few_lane % FEW + 1).astype(F32)
            )
        feeds_ref[...] = feeds.astype(BF16)
        pick_low = pick.astype(BF16)
        pick_ref[...] = pick_low
        weight_ref[...] = jnp.broadcast_to(
            jnp.sum(weight, axis=1, keepdims=True), (FEW, LANES)
        )

        tile_row = iota((rows, LANES), 0)
        tile_lane = iota((rows, LANES), 1)
        wanted = (tile_lane >= codes) & (tile_lane < ending) & (tile_lane % CAP == tile_row % CAP)
        for index, ref in enumerate((mine_ref, other_ref)):
            scale = jnp.sum(
                jnp.where(wanted, tiles[index].astype(F32), 0.0), axis=1, keepdims=True
            )
            part = slice(index * rows, (index + 1) * rows)
            scaled_ref[part, :] = (ref[:, :side].astype(F32) * scale).astype(BF16)
            rows_ref[part, :] = (x_mine_ref, x_other_ref)[index][...]
        y_few_ref[...] = jnp.zeros((FEW, width), BF16)
        blocks = side // columns
        spot = pl.ds(pl.multiple_of(place % blocks * columns, columns), columns)
        column = jnp.concatenate([mine_ref[:, spot], other_ref[:, spot]], 0).astype(F32)
        column = jnp.where(place < blocks, column, pltpu.roll(column, 2 * rows - CAP, 0))
        column_ref[...] = column.astype(BF16)
        rows_few_ref[...] = matmul(pick_low, column_ref[...])
        x_lane = iota((units, 2 * rows), 1) % ROWS < CAP

        def whole_rows(weight_ref, ref):
            return project(weight_ref[:, :side], ref[...]) + pltpu.roll(
                project(weight_ref[:, side:], ref[...]), 2 * rows - CAP, 1
            )

        grad = whole_rows(w_down_ref, scaled_ref)
        gate_pre = whole_rows(w_gate_ref, rows_ref)
        up_pre = whole_rows(w_up_ref, rows_ref)
        sig = 1.0 / (1.0 + jnp.exp(-gate_pre))
        act = jnp.where(x_lane, gate_pre * sig, 0.0)
        slope = jnp.where(x_lane, up_pre * sig * (1.0 + gate_pre * (1.0 - sig)), 0.0)
        act_ref[...] = act
        slope_ref[...] = slope
        hidden_ref[...] = (act * up_pre).astype(BF16)
        gate_ref[...] = (grad * slope).astype(BF16)
        up_ref[...] = (grad * act).astype(BF16)

        def exact(value):
            return lax.dot_general(
                value,
                pick,
                (((1,), (1,)), ((), ())),
                precision=lax.Precision.HIGHEST,
                preferred_element_type=F32,
            )

        act_few_ref[...] = exact(act_ref[...])
        slope_few_ref[...] = exact(slope_ref[...])
        hidden_few_ref[...] = project(hidden_ref[...], pick_low).astype(BF16)
        gate_few = project(gate_ref[...], pick_low).astype(BF16)
        up_few = project(up_ref[...], pick_low).astype(BF16)
        gate_few_ref[...] = gate_few
        up_few_ref[...] = up_few
        share = (sum_rows(gate_few, w_gate_ref[...]) + sum_rows(up_few, w_up_ref[...])).astype(BF16)
        for index in range(devices):
            share_ref[index] = share[:, index * columns : (index + 1) * columns]

    shapes = [
        ((FEW, sections * FEW), BF16),
        ((FEW, ROWS * devices), BF16),
        ((FEW, LANES), F32),
        ((devices, LANES), F32),
        ((2 * rows, columns), BF16),
        ((2 * rows, side), BF16),
        ((2 * rows, side), BF16),
        ((units, 2 * rows), F32),
        ((units, 2 * rows), F32),
        ((units, 2 * rows), BF16),
        ((units, 2 * rows), BF16),
        ((units, 2 * rows), BF16),
        ((units, FEW), F32),
        ((units, FEW), F32),
        ((units, FEW), BF16),
        ((units, FEW), BF16),
        ((units, FEW), BF16),
        ((FEW, columns), F32),
        ((FEW, width), BF16),
        ((devices, FEW, columns), BF16),
    ]
    smem = pl.BlockSpec(memory_space=pltpu.SMEM)
    return pl.pallas_call(
        kernel,
        compiler_params=grant(28),
        in_specs=[smem] + [whole_spec(value.shape) for value in (x_mine, x_other, mine, other)] + [whole_spec(w_gate.shape)] * 3,
        out_specs=[whole_spec(shape) for shape, _ in shapes] + [smem],
        out_shape=[jax.ShapeDtypeStruct(shape, dtype) for shape, dtype in shapes]
        + [jax.ShapeDtypeStruct((2,), jnp.int32)],
    )(where, x_mine, x_other, mine, other, w_gate, w_up, w_down)


def chain_step(last, y_blocks, act_few, slope_few, w_gate, w_up, w_down):
    devices, size, columns = y_blocks.shape
    units, width = w_gate.shape

    def kernel(
        last_ref,
        blocks_ref,
        act_ref,
        slope_ref,
        w_gate_ref,
        w_up_ref,
        w_down_ref,
        y_ref,
        gate_few_ref,
        up_few_ref,
        share_ref,
    ):
        for index in range(devices):
            y_ref[:, index * columns : (index + 1) * columns] = blocks_ref[index]
        grad = project(w_down_ref[...], y_ref[...])
        gate_few = (grad * slope_ref[...]).astype(BF16)
        up_few = (grad * act_ref[...]).astype(BF16)
        gate_few_ref[...] = gate_few
        up_few_ref[...] = up_few

        @pl.when(last_ref[0] == 0)
        def _():
            share = sum_rows(gate_few, w_gate_ref[...])
            share = (share + sum_rows(up_few, w_up_ref[...])).astype(BF16)
            for index in range(devices):
                share_ref[index] = share[:, index * columns : (index + 1) * columns]

    shapes = [(size, width), (units, size), (units, size), (devices, size, columns)]
    return pl.pallas_call(
        kernel,
        compiler_params=grant(16),
        in_specs=[pl.BlockSpec(memory_space=pltpu.SMEM)]
        + [whole_spec(value.shape) for value in (y_blocks, act_few, slope_few)]
        + [whole_spec(w_gate.shape)] * 3,
        out_specs=[whole_spec(shape) for shape in shapes],
        out_shape=[jax.ShapeDtypeStruct(shape, BF16) for shape in shapes],
    )(last, y_blocks, act_few, slope_few, w_gate, w_up, w_down)


def merge_chains(pick, gate, up, hidden, gate_few, up_few, w_gate, w_up):
    units, width = w_gate.shape
    lanes = gate.shape[1]
    rows = lanes // 2

    def kernel(
        pick_ref,
        gate_ref,
        up_ref,
        hidden_ref,
        gate_few_ref,
        up_few_ref,
        w_gate_ref,
        w_up_ref,
        gate_out,
        up_out,
        hidden_out,
        mine_out,
        other_out,
    ):
        pick_low = pick_ref[...]
        keep = jnp.sum(pick_low.astype(F32), axis=0, keepdims=True) == 0.0
        gate_all = jnp.where(keep, gate_ref[...].astype(F32), matmul(gate_few_ref[...], pick_low))
        up_all = jnp.where(keep, up_ref[...].astype(F32), matmul(up_few_ref[...], pick_low))
        kept = jnp.where(keep, hidden_ref[...].astype(F32), 0.0)
        for ref, value in ((gate_out, gate_all), (up_out, up_all), (hidden_out, kept)):
            ref[0] = value.astype(BF16)
            ref[1] = pltpu.roll(value, CAP, 1).astype(BF16)
        side = width // 2

        def shares(ref, weight_ref):
            return sum_rows(ref[0], weight_ref[:, :side]) + sum_rows(ref[1], weight_ref[:, side:])

        share = (shares(gate_out, w_gate_ref) + shares(up_out, w_up_ref)).astype(BF16)
        mine_out[...] = share[:rows]
        other_out[...] = share[rows:]

    shapes = [(2, units, lanes)] * 3 + [(rows, width // 2)] * 2
    values = (pick, gate, up, hidden, gate_few, up_few)
    return pl.pallas_call(
        kernel,
        compiler_params=grant(16),
        in_specs=[whole_spec(value.shape) for value in values] + [whole_spec(w_gate.shape)] * 2,
        out_specs=[whole_spec(shape) for shape in shapes],
        out_shape=[jax.ShapeDtypeStruct(shape, BF16) for shape in shapes],
    )(*values, w_gate, w_up)


def weight_gradients(x_rows, y_rows, gate, up, hidden, hidden_few, y_few):
    _, units, lanes = gate.shape
    few, width = y_few.shape
    block = 512
    per_side = x_rows.shape[1] // block

    def kernel(x_ref, y_ref, gate_ref, up_ref, h_ref, hf_ref, yf_ref, gate_out, up_out, down_out):
        gate_out[...] = matmul(gate_ref[0], x_ref[...]).astype(BF16)
        up_out[...] = matmul(up_ref[0], x_ref[...]).astype(BF16)
        down_out[...] = (
            matmul(h_ref[0], y_ref[...]) + matmul(hf_ref[...], yf_ref[...])
        ).astype(BF16)

    half = pl.BlockSpec((1, units, lanes), lambda i: (i // per_side, 0, 0))
    side = pl.BlockSpec((lanes, block), lambda i: (0, i % per_side))
    across = lambda count: pl.BlockSpec((count, block), lambda i: (0, i))
    return pl.pallas_call(
        kernel,
        compiler_params=grant(16),
        grid=(width // block,),
        in_specs=[side, side, half, half, half]
        + [pl.BlockSpec(hidden_few.shape, lambda i: (0, 0)), across(few)],
        out_specs=[across(units)] * 3,
        out_shape=[jax.ShapeDtypeStruct((units, width), BF16)] * 3,
    )(x_rows, y_rows, gate, up, hidden, hidden_few, y_few)


def prepare(ids, weights, out_grad, sections):
    count, part_width = out_grad.shape
    codes = sections * CAP

    def kernel(ids_ref, weights_ref, grad_ref, sent_ref, select_ref, weight_ref):
        live = as_float(ids_ref[...] == 0)
        weight = jnp.sum(live * weights_ref[...], axis=0, keepdims=True)
        live = jnp.sum(live, axis=0, keepdims=True)
        row = iota((count, count), 0)
        col = iota((count, count), 1)
        slot = matmul(jnp.broadcast_to(live, (8, count)), as_float(row < col))[:1]
        slot = jnp.where(live > 0, slot, -1.0)
        at_slot = as_float(slot == row.astype(F32))
        index = iota((8, count), 1).astype(F32) + 1.0
        token = project(index, at_slot) - 1.0
        tile = jnp.concatenate([token, jnp.zeros((8, part_width - count), F32)], 1).astype(BF16)
        sent_ref[:count, :] = grad_ref[...]
        sent_ref[count:, :] = tile
        select_ref[...] = at_slot[:8].astype(BF16)
        parts = jnp.zeros((8, LANES), F32)
        remainder = weight
        for part in range(PARTS):
            piece = remainder.astype(BF16).astype(F32)
            remainder = remainder - piece
            moved = as_float((slot + (codes + part * CAP) == row.astype(F32)) & (slot >= 0))
            parts = parts + project(jnp.broadcast_to(piece, (8, count)), moved)
        weight_ref[...] = parts

    shapes = [((count + 8, part_width), BF16), ((8, count), BF16), ((8, LANES), F32)]
    return pl.pallas_call(
        kernel,
        compiler_params=grant(8),
        in_specs=[whole_spec(value.shape) for value in (ids, weights, out_grad)],
        out_specs=[whole_spec(shape) for shape, _ in shapes],
        out_shape=[jax.ShapeDtypeStruct(shape, dtype) for shape, dtype in shapes],
    )(ids, weights, out_grad)


def halves_of(select):
    low = select.astype(F32)
    return low, pltpu.roll(low, CAP, 0)


def pack_inputs(select, tokens, chips):
    side = tokens.shape[1] // 2

    def kernel(select_ref, tokens_ref, packed_ref):
        low, high = halves_of(select_ref[...])
        rows = (
            matmul(low.astype(BF16), tokens_ref[:, :side])
            + matmul(high.astype(BF16), tokens_ref[:, side:])
        ).astype(BF16)
        for chip in range(chips):
            packed_ref[chip] = rows

    shape = (chips, ROWS, side)
    return pl.pallas_call(
        kernel,
        compiler_params=grant(8),
        in_specs=[whole_spec(select.shape), whole_spec(tokens.shape)],
        out_specs=whole_spec(shape),
        out_shape=jax.ShapeDtypeStruct(shape, BF16),
    )(select, tokens)


def shifts_of(sections):
    return [0] + [way * d for d in range(1, sections // 2) for way in (1, -1)] + [sections // 2]


def pack(where, parts, select, weight, chips):
    sections = len(parts)
    tall, part_width = parts[0].shape
    count = tall - 8
    side = sections * part_width // 2
    codes = sections * CAP
    shifts = shifts_of(sections)

    def kernel(where_ref, *refs):
        part_refs = refs[:sections]
        select_ref, weight_ref, packed_ref, token_ref, rows_ref, tokens_ref = refs[sections:]
        section = where_ref[0]
        low, high = halves_of(select_ref[...])
        rows_ref[...] = jnp.zeros((ROWS, side), F32)
        for shift, ref in zip(shifts, part_refs):
            source = (section + sections - shift) % sections
            chosen = jnp.where(source < sections // 2, low, high).astype(BF16)
            start = source % (sections // 2) * part_width
            spot = pl.ds(pl.multiple_of(start, part_width), part_width)
            rows_ref[:, spot] += matmul(chosen, ref[:count, :])
            tokens_ref[pl.ds(source, 1), :] = ref[count:, :LANES].astype(F32)[:1]
        tokens = tokens_ref[...]
        row = iota((LANES, LANES), 0)
        col = iota((LANES, LANES), 1)
        spread = matmul(tokens, as_float((row < CAP) & (col % CAP == row)))
        lane = iota((sections, LANES), 1)
        layer = iota((sections, LANES), 0)
        pick_lane = lambda size: jnp.sum(
            jnp.where(lane // size == layer, spread, 0.0), axis=0, keepdims=True
        )
        flat = pick_lane(CAP)
        one_lane = lane[:1]
        flat = jnp.where(one_lane < codes, flat, -1.0)
        times = jnp.zeros((1, LANES), F32)
        for slot in range(CAP):
            times = times + jnp.sum(
                as_float(tokens[:, slot : slot + 1] == flat), axis=0, keepdims=True
            )
        times = jnp.where(flat >= 0, times, 0.0)
        code = jnp.where(times > 1, flat, -1.0)
        note = jnp.where(one_lane < codes, code, weight_ref[:1])
        note = jnp.where(one_lane == codes + PARTS * CAP, jnp.max(times), note)
        note = jnp.broadcast_to(note, (ROWS, LANES)).astype(BF16)
        token_ref[...] = jnp.broadcast_to(pick_lane(2 * CAP), (8, LANES))
        rows = rows_ref[...].astype(BF16)
        for chip in range(chips):
            packed_ref[chip, :, :side] = rows
            packed_ref[chip, :, side:] = note

    shapes = [((chips, ROWS, side + LANES), BF16), ((8, LANES), F32)]
    return pl.pallas_call(
        kernel,
        compiler_params=grant(8),
        in_specs=[pl.BlockSpec(memory_space=pltpu.SMEM)]
        + [whole_spec(value.shape) for value in (*parts, select, weight)],
        out_specs=[whole_spec(shape) for shape, _ in shapes],
        out_shape=[jax.ShapeDtypeStruct(shape, dtype) for shape, dtype in shapes],
        scratch_shapes=[pltpu.VMEM((ROWS, side), F32), pltpu.VMEM((sections, LANES), F32)],
    )(where, *parts, select, weight)


def assemble(where, tokens, parts, back):
    sections = len(parts)
    tall, part_width = parts[0].shape
    count = tall - 8
    rows, side = back.shape
    shifts = shifts_of(sections)

    def kernel(where_ref, token_ref, *refs):
        part_refs = refs[:sections]
        back_ref, out_ref = refs[sections:]
        section = where_ref[0]
        lane = iota((count, rows), 1)
        taken = as_float(
            (token_ref[:1, :rows] == iota((count, rows), 0).astype(F32))
            & (lane // (2 * CAP) >= section)
        )
        second = as_float(lane // CAP % 2 == 1)
        for shift, ref in zip(shifts, part_refs):
            source = (section + sections - shift) % sections
            here = jnp.where(source < sections // 2, 1.0 - second, second) * taken
            near = pl.multiple_of(source % (sections // 2) * part_width, part_width)
            added = matmul(here.astype(BF16), back_ref[:, pl.ds(near, part_width)])
            far = pl.multiple_of(source * part_width, part_width)
            out_ref[:, pl.ds(far, part_width)] = (
                ref[:count, :].astype(F32) + added
            ).astype(BF16)

    shape = (count, 2 * side)
    return pl.pallas_call(
        kernel,
        compiler_params=grant(8),
        in_specs=[pl.BlockSpec(memory_space=pltpu.SMEM)]
        + [whole_spec(value.shape) for value in (tokens, *parts, back)],
        out_specs=whole_spec(shape),
        out_shape=jax.ShapeDtypeStruct(shape, BF16),
    )(where, tokens, *parts, back)


def on_device(saved_inputs, expert_ids, gate_weights, out_grad, gate_w, up_w, down_w):
    sections = lax.axis_size("section")
    devices = lax.axis_size("ep")
    chips = devices // 2
    section = lax.axis_index("section")
    place = lax.axis_index("ep")
    core = place % 2
    groups = [[2 * chip + k for chip in range(chips)] for k in range(2)]
    width = saved_inputs.shape[2]
    columns = width // devices
    slots = devices * CAP
    tokens = saved_inputs[0]
    token_count = tokens.shape[0]
    w_gate = gate_w[0]
    w_up = up_w[0]
    w_down = down_w[0]

    where = jnp.stack([section, core, place]).astype(jnp.int32)
    sent, select, slot_weight = prepare(
        expert_ids[0].T, gate_weights[0].T, out_grad, sections
    )

    def around(value, shift):
        pairs = [(i, (i + shift) % sections) for i in range(sections)]
        return lax.ppermute(value, "section", pairs)

    parts = [sent]
    above = below = sent
    for shift in range(1, sections // 2 + 1):
        below = around(below, 1)
        parts.append(below)
        if shift < sections // 2:
            above = around(above, -1)
            parts.append(above)
    x_mine = exchange(pack_inputs(select, tokens, chips), "ep", groups)
    x_mine, parts, select, slot_weight, where = lax.optimization_barrier(
        (x_mine, parts, select, slot_weight, where)
    )
    x_other = from_partner(x_mine, devices)
    packed, all_tokens = pack(where, parts, select, slot_weight, chips)
    y_mine = exchange(packed, "ep", groups)
    y_other = from_partner(y_mine, devices)
    flat = lambda value: value.reshape(chips * ROWS, value.shape[2])

    (
        feeds_few,
        pick_few,
        weight_few,
        notes,
        column,
        x_rows,
        y_rows,
        act,
        slope,
        hidden,
        gate_first,
        up_first,
        act_few,
        slope_few,
        hidden_few,
        gate_few,
        up_few,
        rows_few,
        y_few,
        share_few,
        counts,
    ) = first_pass(
        where,
        flat(x_mine),
        flat(x_other),
        flat(y_mine),
        flat(y_other),
        w_gate,
        w_up,
        w_down,
        sections,
    )
    chain_count = counts[0]
    trips = counts[1]
    def slow_plan(size):
        layer_index = jnp.arange(sections, dtype=jnp.int32)
        index = jnp.arange(size, dtype=jnp.int32)
        in_chain = (notes[:, : sections * CAP] >= 0).reshape(devices, sections, CAP)
        flags = jnp.swapaxes(in_chain, 0, 1).reshape(sections, slots)
        within = notes[:, : sections * CAP].astype(jnp.int32).reshape(devices, sections, CAP)
        base = token_count * jnp.arange(devices, dtype=jnp.int32)[:, None, None]
        token = jnp.swapaxes(within + base + 1, 0, 1).reshape(sections, slots)
        place = jnp.cumsum(flags.astype(jnp.int32), axis=1) - 1
        listed = flags[:, None, :] & (place[:, None, :] == index[None, :, None])
        tokens_of = jnp.sum(jnp.where(listed, token[:, None, :], 0), axis=2)
        own_token = lax.dynamic_index_in_dim(tokens_of, section, 0, keepdims=False)
        own = lax.dynamic_index_in_dim(listed, section, 0, keepdims=False)
        parts = notes[:, sections * CAP : (sections + PARTS) * CAP].reshape(devices, PARTS, CAP)
        weight = jnp.sum(jnp.where(own, jnp.sum(parts, axis=1).reshape(1, slots), 0.0), axis=1)
        feeds = (
            (own_token[:, None, None] == tokens_of[None])
            & (own_token[:, None, None] > 0)
            & (layer_index[None, :, None] > section)
        )
        halves = own.reshape(size, 2, chips, CAP)
        halves = jnp.where(core == 0, halves, halves[:, ::-1])
        halves = jnp.concatenate([halves, jnp.zeros_like(halves)], 3)
        return (
            feeds.reshape(size, sections * size).astype(BF16),
            halves.reshape(size, devices * ROWS).astype(BF16),
            jnp.broadcast_to(weight[:, None], (size, LANES)),
        )

    def slow_start(size):
        feeds, pick, weight = slow_plan(size)
        exact = lambda value: lax.dot_general(
            value,
            pick.astype(F32),
            (((1,), (1,)), ((), ())),
            precision=lax.Precision.HIGHEST,
        )
        gate = project(gate_first, pick).astype(BF16)
        up = project(up_first, pick).astype(BF16)
        share = (sum_rows(gate, w_gate) + sum_rows(up, w_up)).astype(BF16)
        return (
            feeds,
            pick,
            weight,
            exact(act),
            exact(slope),
            project(hidden, pick).astype(BF16),
            gate,
            up,
            matmul(pick, column),
            jnp.zeros((size, width), BF16),
            jnp.swapaxes(share.reshape(size, devices, columns), 0, 1),
        )

    def finish(size):
        if size == FEW:
            start = (
                feeds_few,
                pick_few,
                weight_few,
                act_few,
                slope_few,
                hidden_few,
                gate_few,
                up_few,
                rows_few,
                y_few,
                share_few,
            )
        else:
            start = slow_start(size)
        feeds, pick, weight, act_rows, slope_rows, hidden_rows = start[:6]
        first_rows = start[8]

        def more(state):
            return state[0] < trips

        def step(state):
            trip = state[0] + 1
            last = (trip >= trips).astype(jnp.int32).reshape(1)
            share, trip, last = lax.optimization_barrier((state[4], trip, last))
            summed = jnp.sum(exchange(share, "ep").astype(F32), axis=0)
            summed = lax.reduce_precision(summed, 8, 7).astype(BF16)
            layers = exchange(repeated(summed, sections), "section")
            above_rows = first_rows + matmul(feeds, layers.reshape(sections * size, columns))
            above_rows = lax.reduce_precision(above_rows, 8, 7)
            y_part = (weight * above_rows).astype(BF16)
            blocks = exchange(repeated(y_part, devices), "ep")
            y, gate, up, share = chain_step(last, blocks, act_rows, slope_rows, w_gate, w_up, w_down)
            return (trip, y, gate, up, share)

        state = (jnp.int32(0), start[9], start[6], start[7], start[10])
        _, y, gate, up, _ = lax.while_loop(more, step, state)
        gate, up, hidden_kept, share_mine, share_other = merge_chains(
            pick, gate_first, up_first, hidden, gate, up, w_gate, w_up
        )

        theirs = from_partner(share_other, devices)
        chip_sum = (share_mine.astype(F32) + theirs.astype(F32)).astype(BF16)
        tiles = exchange(chip_sum.reshape(chips, ROWS, width // 2), "ep", groups)
        back = lax.reduce_precision(jnp.sum(tiles.astype(F32), axis=0), 8, 7).astype(BF16)
        all_back = exchange(repeated(back, sections), "section")
        grads = weight_gradients(
            x_rows, y_rows, gate, up, hidden_kept, hidden_rows, y
        )
        result = assemble(where, all_tokens, parts, all_back.reshape(sections * ROWS, width // 2))
        return (result, *grads)

    outputs = lax.cond(chain_count <= FEW, lambda: finish(FEW), lambda: finish(slots))
    return tuple(output[None] for output in outputs)


def solution(mesh):
    by_rows = P("section", "ep", None)
    return jax.shard_map(
        on_device,
        mesh=mesh,
        in_specs=(by_rows, by_rows, by_rows, P("ep", "section"), by_rows, by_rows, by_rows),
        out_specs=(by_rows, by_rows, by_rows, by_rows),
        check_vma=False,
    )
```

```python
import jax
import jax.numpy as jnp
from jax import lax
from jax.experimental import pallas as pl
from jax.experimental.pallas import tpu as pltpu
from jax.sharding import PartitionSpec as P


CAP = 4
ROWS = 2 * CAP
FEW = 16
PARTS = 3
LANES = 128
F32 = jnp.float32
BF16 = jnp.bfloat16


def exchange(blocks, axis, groups=None):
    return lax.all_to_all(blocks, axis, 0, 0, tiled=True, axis_index_groups=groups)


def repeated(value, count):
    return jnp.broadcast_to(value[None], (count, *value.shape))


def from_partner(value, devices):
    return lax.ppermute(value, "ep", [(i, i ^ 1) for i in range(devices)])


def project(row_data, weight):
    return lax.dot_general(
        row_data, weight, (((1,), (1,)), ((), ())), preferred_element_type=F32
    )


def matmul(left, right):
    return jnp.dot(left, right, preferred_element_type=F32)


def sum_rows(left, right):
    return lax.dot_general(
        left, right, (((0,), (0,)), ((), ())), preferred_element_type=F32
    )


def iota(shape, dim):
    return lax.broadcasted_iota(jnp.int32, shape, dim)


def grant(mebibytes):
    return pltpu.CompilerParams(vmem_limit_bytes=mebibytes << 20)


def as_float(mask):
    return jnp.where(mask, 1.0, 0.0)


def whole_spec(shape):
    return pl.BlockSpec(shape, lambda: (0,) * len(shape))


def first_pass(where, x_mine, x_other, mine, other, w_gate, w_up, w_down, sections):
    half = mine.shape[0] // ROWS
    rows = half * ROWS
    side = x_mine.shape[1]
    devices = 2 * half
    codes = sections * CAP
    ending = codes + PARTS * CAP
    units, width = w_gate.shape
    columns = width // devices

    def kernel(
        where_ref,
        x_mine_ref,
        x_other_ref,
        mine_ref,
        other_ref,
        w_gate_ref,
        w_up_ref,
        w_down_ref,
        feeds_ref,
        pick_ref,
        weight_ref,
        note_ref,
        column_ref,
        rows_ref,
        scaled_ref,
        act_ref,
        slope_ref,
        hidden_ref,
        gate_ref,
        up_ref,
        act_few_ref,
        slope_few_ref,
        hidden_few_ref,
        gate_few_ref,
        up_few_ref,
        rows_few_ref,
        y_few_ref,
        share_ref,
        fits_ref,
        trips_ref,
    ):
        section = where_ref[0]
        core = where_ref[1]
        place = where_ref[2]

        lead = as_float(iota((half, rows), 1) == ROWS * iota((half, rows), 0)).astype(BF16)
        tiles = [ref[:, side:] for ref in (mine_ref, other_ref)]
        near = matmul(lead, tiles[0])
        far = matmul(lead, tiles[1])
        note = jnp.concatenate([jnp.where(core == 0, near, far), jnp.where(core == 0, far, near)], 0)
        note_ref[...] = note
        lane = iota((devices, LANES), 1)
        code = jnp.where(lane < codes, note, -1.0)
        flag = as_float(code >= 0)
        row = iota((LANES, LANES), 0)
        col = iota((LANES, LANES), 1)
        same_layer = row // CAP == col // CAP
        per_layer = matmul(flag, as_float(same_layer))
        longest = jnp.max(jnp.sum(per_layer, axis=0, keepdims=True))
        fits_ref[0] = (longest <= FEW).astype(jnp.int32)
        most = jnp.max(jnp.where(lane == codes + PARTS * CAP, note, 0.0))
        trips_ref[0] = most.astype(jnp.int32) - 1
        before = as_float(iota((devices, devices), 1) < iota((devices, devices), 0))
        rank = matmul(before, per_layer) + matmul(flag, as_float(same_layer & (row < col)))
        rank = (rank + 1.0) * flag
        token = (code + 1.0) * flag
        owned = as_float(iota((8, LANES), 1) == iota((8, LANES), 0) + CAP * section)
        own_rank = project(owned, rank)
        own_token = project(owned, token)
        entry = iota((FEW, devices), 0).astype(F32) + 1.0
        device = iota((devices, 2 * rows), 0)
        spot = iota((devices, 2 * rows), 1)
        home = rows * ((device // half + core) % 2) + ROWS * (device % half)
        held = jnp.zeros((FEW, 1), F32)
        weight = jnp.zeros((FEW, LANES), F32)
        groups = jnp.zeros((FEW, devices), F32)
        pick = jnp.zeros((FEW, 2 * rows), F32)
        few_lane = iota((FEW, LANES), 1)
        for slot in range(CAP):
            here = as_float(own_rank[slot : slot + 1] == entry)
            groups = groups + here
            held = held + jnp.sum(here * own_token[slot : slot + 1], axis=1, keepdims=True)
            part = matmul(here, note)
            wanted = (few_lane >= codes) & (few_lane < ending) & (few_lane % CAP == slot)
            weight = weight + jnp.where(wanted, part, 0.0)
            pick = pick + matmul(here, as_float(spot == home + slot))
        near_rank = matmul(groups, rank)
        near_token = matmul(groups, token)
        match = (near_token == held) & (near_token > 0) & (few_lane // CAP > section)
        source = jnp.where(match & (few_lane < codes), near_rank, 0.0)
        feeds = jnp.zeros((FEW, LANES), F32)
        for slot in range(CAP):
            spread = as_float((row // CAP == col // FEW) & (row % CAP == slot))
            feeds = feeds + as_float(
                matmul(source, spread) == (few_lane % FEW + 1).astype(F32)
            )
        feeds_ref[...] = feeds.astype(BF16)
        pick_low = pick.astype(BF16)
        pick_ref[...] = pick_low
        weight_ref[...] = jnp.broadcast_to(
            jnp.sum(weight, axis=1, keepdims=True), (FEW, LANES)
        )

        tile_row = iota((rows, LANES), 0)
        tile_lane = iota((rows, LANES), 1)
        wanted = (tile_lane >= codes) & (tile_lane < ending) & (tile_lane % CAP == tile_row % CAP)
        for index, ref in enumerate((mine_ref, other_ref)):
            scale = jnp.sum(
                jnp.where(wanted, tiles[index].astype(F32), 0.0), axis=1, keepdims=True
            )
            part = slice(index * rows, (index + 1) * rows)
            scaled_ref[part, :] = (ref[:, :side].astype(F32) * scale).astype(BF16)
            rows_ref[part, :] = (x_mine_ref, x_other_ref)[index][...]
        y_few_ref[...] = jnp.zeros((FEW, width), BF16)
        blocks = side // columns
        spot = pl.ds(pl.multiple_of(place % blocks * columns, columns), columns)
        column = jnp.concatenate([mine_ref[:, spot], other_ref[:, spot]], 0).astype(F32)
        column = jnp.where(place < blocks, column, pltpu.roll(column, 2 * rows - CAP, 0))
        column_ref[...] = column.astype(BF16)
        rows_few_ref[...] = matmul(pick_low, column_ref[...])
        x_lane = iota((units, 2 * rows), 1) % ROWS < CAP

        def whole_rows(weight_ref, ref):
            return project(weight_ref[:, :side], ref[...]) + pltpu.roll(
                project(weight_ref[:, side:], ref[...]), 2 * rows - CAP, 1
            )

        grad = whole_rows(w_down_ref, scaled_ref)
        gate_pre = whole_rows(w_gate_ref, rows_ref)
        up_pre = whole_rows(w_up_ref, rows_ref)
        sig = 1.0 / (1.0 + jnp.exp(-gate_pre))
        act = jnp.where(x_lane, gate_pre * sig, 0.0)
        slope = jnp.where(x_lane, up_pre * sig * (1.0 + gate_pre * (1.0 - sig)), 0.0)
        act_ref[...] = act
        slope_ref[...] = slope
        hidden_ref[...] = (act * up_pre).astype(BF16)
        gate_ref[...] = (grad * slope).astype(BF16)
        up_ref[...] = (grad * act).astype(BF16)

        def exact(value):
            total = jnp.zeros((units, FEW), F32)
            for _ in range(PARTS):
                piece = value.astype(BF16)
                total = total + project(piece, pick_low)
                value = value - piece.astype(F32)
            return total

        act_few_ref[...] = exact(act_ref[...])
        slope_few_ref[...] = exact(slope_ref[...])
        hidden_few_ref[...] = project(hidden_ref[...], pick_low).astype(BF16)
        gate_few = project(gate_ref[...], pick_low).astype(BF16)
        up_few = project(up_ref[...], pick_low).astype(BF16)
        gate_few_ref[...] = gate_few
        up_few_ref[...] = up_few
        share = (sum_rows(gate_few, w_gate_ref[...]) + sum_rows(up_few, w_up_ref[...])).astype(BF16)
        for index in range(devices):
            share_ref[index] = share[:, index * columns : (index + 1) * columns]

    shapes = [
        ((FEW, sections * FEW), BF16),
        ((FEW, ROWS * devices), BF16),
        ((FEW, LANES), F32),
        ((devices, LANES), F32),
        ((2 * rows, columns), BF16),
        ((2 * rows, side), BF16),
        ((2 * rows, side), BF16),
        ((units, 2 * rows), F32),
        ((units, 2 * rows), F32),
        ((units, 2 * rows), BF16),
        ((units, 2 * rows), BF16),
        ((units, 2 * rows), BF16),
        ((units, FEW), F32),
        ((units, FEW), F32),
        ((units, FEW), BF16),
        ((units, FEW), BF16),
        ((units, FEW), BF16),
        ((FEW, columns), F32),
        ((FEW, width), BF16),
        ((devices, FEW, columns), BF16),
    ]
    smem = pl.BlockSpec(memory_space=pltpu.SMEM)
    return pl.pallas_call(
        kernel,
        compiler_params=grant(28),
        in_specs=[smem] + [whole_spec(value.shape) for value in (x_mine, x_other, mine, other)] + [whole_spec(w_gate.shape)] * 3,
        out_specs=[whole_spec(shape) for shape, _ in shapes] + [smem] * 2,
        out_shape=[jax.ShapeDtypeStruct(shape, dtype) for shape, dtype in shapes]
        + [jax.ShapeDtypeStruct((1,), jnp.int32)] * 2,
    )(where, x_mine, x_other, mine, other, w_gate, w_up, w_down)


def chain_rows(layers, feeds, first_rows, weight, devices):
    sections = layers.shape[0]
    size, columns = first_rows.shape

    def kernel(layers_ref, feeds_ref, first_ref, weight_ref, out_ref):
        rows = first_ref[...]
        for layer in range(sections - 1, 0, -1):
            feed = feeds_ref[:, layer * size : (layer + 1) * size]
            added = matmul(feed, layers_ref[layer, :size, :]) + matmul(
                feed, layers_ref[layer, size:, :]
            )
            rows = (rows + added).astype(BF16).astype(F32)
        rows = (weight_ref[...] * rows).astype(BF16)
        for device in range(devices):
            out_ref[device] = rows

    values = (layers, feeds, first_rows, weight)
    shape = (devices, size, columns)
    return pl.pallas_call(
        kernel,
        compiler_params=grant(8),
        in_specs=[whole_spec(value.shape) for value in values],
        out_specs=whole_spec(shape),
        out_shape=jax.ShapeDtypeStruct(shape, BF16),
    )(*values)


def chain_step(last, y_blocks, act_few, slope_few, w_gate, w_up, w_down):
    devices, size, columns = y_blocks.shape
    units, width = w_gate.shape

    def kernel(
        last_ref,
        blocks_ref,
        act_ref,
        slope_ref,
        w_gate_ref,
        w_up_ref,
        w_down_ref,
        y_ref,
        gate_few_ref,
        up_few_ref,
        share_ref,
    ):
        for index in range(devices):
            y_ref[:, index * columns : (index + 1) * columns] = blocks_ref[index]
        grad = project(w_down_ref[...], y_ref[...])
        gate_few = (grad * slope_ref[...]).astype(BF16)
        up_few = (grad * act_ref[...]).astype(BF16)
        gate_few_ref[...] = gate_few
        up_few_ref[...] = up_few

        @pl.when(last_ref[0] == 0)
        def _():
            share = sum_rows(gate_few, w_gate_ref[...])
            share = (share + sum_rows(up_few, w_up_ref[...])).astype(BF16)
            for index in range(devices):
                share_ref[index] = share[:, index * columns : (index + 1) * columns]

    shapes = [(size, width), (units, size), (units, size), (devices, size, columns)]
    return pl.pallas_call(
        kernel,
        compiler_params=grant(16),
        in_specs=[pl.BlockSpec(memory_space=pltpu.SMEM)]
        + [whole_spec(value.shape) for value in (y_blocks, act_few, slope_few)]
        + [whole_spec(w_gate.shape)] * 3,
        out_specs=[whole_spec(shape) for shape in shapes],
        out_shape=[jax.ShapeDtypeStruct(shape, BF16) for shape in shapes],
    )(last, y_blocks, act_few, slope_few, w_gate, w_up, w_down)


def merge_chains(pick, gate, up, hidden, gate_few, up_few, w_gate, w_up):
    units, width = w_gate.shape
    lanes = gate.shape[1]
    rows = lanes // 2

    def kernel(
        pick_ref,
        gate_ref,
        up_ref,
        hidden_ref,
        gate_few_ref,
        up_few_ref,
        w_gate_ref,
        w_up_ref,
        gate_out,
        up_out,
        hidden_out,
        mine_out,
        other_out,
    ):
        pick_low = pick_ref[...]
        keep = jnp.sum(pick_low.astype(F32), axis=0, keepdims=True) == 0.0
        gate_all = jnp.where(keep, gate_ref[...].astype(F32), matmul(gate_few_ref[...], pick_low))
        up_all = jnp.where(keep, up_ref[...].astype(F32), matmul(up_few_ref[...], pick_low))
        kept = jnp.where(keep, hidden_ref[...].astype(F32), 0.0)
        for ref, value in ((gate_out, gate_all), (up_out, up_all), (hidden_out, kept)):
            ref[0] = value.astype(BF16)
            ref[1] = pltpu.roll(value, CAP, 1).astype(BF16)
        side = width // 2

        def shares(ref, weight_ref):
            return sum_rows(ref[0], weight_ref[:, :side]) + sum_rows(ref[1], weight_ref[:, side:])

        share = (shares(gate_out, w_gate_ref) + shares(up_out, w_up_ref)).astype(BF16)
        mine_out[...] = share[:rows]
        other_out[...] = share[rows:]

    shapes = [(2, units, lanes)] * 3 + [(rows, width // 2)] * 2
    values = (pick, gate, up, hidden, gate_few, up_few)
    return pl.pallas_call(
        kernel,
        compiler_params=grant(16),
        in_specs=[whole_spec(value.shape) for value in values] + [whole_spec(w_gate.shape)] * 2,
        out_specs=[whole_spec(shape) for shape in shapes],
        out_shape=[jax.ShapeDtypeStruct(shape, BF16) for shape in shapes],
    )(*values, w_gate, w_up)


def weight_gradients(x_rows, y_rows, gate, up, hidden, hidden_few, y_few):
    _, units, lanes = gate.shape
    few, width = y_few.shape
    block = 512
    per_side = x_rows.shape[1] // block

    def kernel(x_ref, y_ref, gate_ref, up_ref, h_ref, hf_ref, yf_ref, gate_out, up_out, down_out):
        gate_out[...] = matmul(gate_ref[0], x_ref[...]).astype(BF16)
        up_out[...] = matmul(up_ref[0], x_ref[...]).astype(BF16)
        down_out[...] = (
            matmul(h_ref[0], y_ref[...]) + matmul(hf_ref[...], yf_ref[...])
        ).astype(BF16)

    half = pl.BlockSpec((1, units, lanes), lambda i: (i // per_side, 0, 0))
    side = pl.BlockSpec((lanes, block), lambda i: (0, i % per_side))
    across = lambda count: pl.BlockSpec((count, block), lambda i: (0, i))
    return pl.pallas_call(
        kernel,
        compiler_params=grant(16),
        grid=(width // block,),
        in_specs=[side, side, half, half, half]
        + [pl.BlockSpec(hidden_few.shape, lambda i: (0, 0)), across(few)],
        out_specs=[across(units)] * 3,
        out_shape=[jax.ShapeDtypeStruct((units, width), BF16)] * 3,
    )(x_rows, y_rows, gate, up, hidden, hidden_few, y_few)


def prepare(ids, weights, out_grad, sections):
    count, part_width = out_grad.shape
    codes = sections * CAP

    def kernel(ids_ref, weights_ref, grad_ref, sent_ref, select_ref, weight_ref):
        live = as_float(ids_ref[...] == 0)
        weight = jnp.sum(live * weights_ref[...], axis=0, keepdims=True)
        live = jnp.sum(live, axis=0, keepdims=True)
        row = iota((count, count), 0)
        col = iota((count, count), 1)
        slot = matmul(jnp.broadcast_to(live, (8, count)), as_float(row < col))[:1]
        slot = jnp.where(live > 0, slot, -1.0)
        at_slot = as_float(slot == row.astype(F32))
        index = iota((8, count), 1).astype(F32) + 1.0
        token = project(index, at_slot) - 1.0
        tile = jnp.concatenate([token, jnp.zeros((8, part_width - count), F32)], 1).astype(BF16)
        sent_ref[:count, :] = grad_ref[...]
        sent_ref[count:, :] = tile
        select_ref[...] = at_slot[:8].astype(BF16)
        parts = jnp.zeros((8, LANES), F32)
        remainder = weight
        for part in range(PARTS):
            piece = remainder.astype(BF16).astype(F32)
            remainder = remainder - piece
            moved = as_float((slot + (codes + part * CAP) == row.astype(F32)) & (slot >= 0))
            parts = parts + project(jnp.broadcast_to(piece, (8, count)), moved)
        weight_ref[...] = parts

    shapes = [((count + 8, part_width), BF16), ((8, count), BF16), ((8, LANES), F32)]
    return pl.pallas_call(
        kernel,
        compiler_params=grant(8),
        in_specs=[whole_spec(value.shape) for value in (ids, weights, out_grad)],
        out_specs=[whole_spec(shape) for shape, _ in shapes],
        out_shape=[jax.ShapeDtypeStruct(shape, dtype) for shape, dtype in shapes],
    )(ids, weights, out_grad)


def halves_of(select):
    low = select.astype(F32)
    return low, pltpu.roll(low, CAP, 0)


def pack_inputs(select, tokens, chips):
    side = tokens.shape[1] // 2

    def kernel(select_ref, tokens_ref, packed_ref):
        low, high = halves_of(select_ref[...])
        rows = (
            matmul(low.astype(BF16), tokens_ref[:, :side])
            + matmul(high.astype(BF16), tokens_ref[:, side:])
        ).astype(BF16)
        for chip in range(chips):
            packed_ref[chip] = rows

    shape = (chips, ROWS, side)
    return pl.pallas_call(
        kernel,
        compiler_params=grant(8),
        in_specs=[whole_spec(select.shape), whole_spec(tokens.shape)],
        out_specs=whole_spec(shape),
        out_shape=jax.ShapeDtypeStruct(shape, BF16),
    )(select, tokens)


def shifts_of(sections):
    return [0] + [way * d for d in range(1, sections // 2) for way in (1, -1)] + [sections // 2]


def pack(where, parts, select, weight, chips):
    sections = len(parts)
    tall, part_width = parts[0].shape
    count = tall - 8
    side = sections * part_width // 2
    codes = sections * CAP
    shifts = shifts_of(sections)

    def kernel(where_ref, *refs):
        part_refs = refs[:sections]
        select_ref, weight_ref, packed_ref, token_ref, rows_ref, tokens_ref = refs[sections:]
        section = where_ref[0]
        low, high = halves_of(select_ref[...])
        rows_ref[...] = jnp.zeros((ROWS, side), F32)
        for shift, ref in zip(shifts, part_refs):
            source = (section + sections - shift) % sections
            chosen = jnp.where(source < sections // 2, low, high).astype(BF16)
            start = source % (sections // 2) * part_width
            spot = pl.ds(pl.multiple_of(start, part_width), part_width)
            rows_ref[:, spot] += matmul(chosen, ref[:count, :])
            tokens_ref[pl.ds(source, 1), :] = ref[count:, :LANES].astype(F32)[:1]
        tokens = tokens_ref[...]
        row = iota((LANES, LANES), 0)
        col = iota((LANES, LANES), 1)
        spread = matmul(tokens, as_float((row < CAP) & (col % CAP == row)))
        lane = iota((sections, LANES), 1)
        layer = iota((sections, LANES), 0)
        pick_lane = lambda size: jnp.sum(
            jnp.where(lane // size == layer, spread, 0.0), axis=0, keepdims=True
        )
        flat = pick_lane(CAP)
        one_lane = lane[:1]
        flat = jnp.where(one_lane < codes, flat, -1.0)
        times = jnp.zeros((1, LANES), F32)
        for slot in range(CAP):
            times = times + jnp.sum(
                as_float(tokens[:, slot : slot + 1] == flat), axis=0, keepdims=True
            )
        times = jnp.where(flat >= 0, times, 0.0)
        code = jnp.where(times > 1, flat, -1.0)
        note = jnp.where(one_lane < codes, code, weight_ref[:1])
        note = jnp.where(one_lane == codes + PARTS * CAP, jnp.max(times), note)
        note = jnp.broadcast_to(note, (ROWS, LANES)).astype(BF16)
        token_ref[...] = jnp.broadcast_to(pick_lane(2 * CAP), (8, LANES))
        rows = rows_ref[...].astype(BF16)
        for chip in range(chips):
            packed_ref[chip, :, :side] = rows
            packed_ref[chip, :, side:] = note

    shapes = [((chips, ROWS, side + LANES), BF16), ((8, LANES), F32)]
    return pl.pallas_call(
        kernel,
        compiler_params=grant(8),
        in_specs=[pl.BlockSpec(memory_space=pltpu.SMEM)]
        + [whole_spec(value.shape) for value in (*parts, select, weight)],
        out_specs=[whole_spec(shape) for shape, _ in shapes],
        out_shape=[jax.ShapeDtypeStruct(shape, dtype) for shape, dtype in shapes],
        scratch_shapes=[pltpu.VMEM((ROWS, side), F32), pltpu.VMEM((sections, LANES), F32)],
    )(where, *parts, select, weight)


def assemble(where, tokens, parts, back):
    sections = len(parts)
    tall, part_width = parts[0].shape
    count = tall - 8
    rows, side = back.shape
    shifts = shifts_of(sections)

    def kernel(where_ref, token_ref, *refs):
        part_refs = refs[:sections]
        back_ref, out_ref = refs[sections:]
        section = where_ref[0]
        lane = iota((count, rows), 1)
        taken = as_float(
            (token_ref[:1, :rows] == iota((count, rows), 0).astype(F32))
            & (lane // (2 * CAP) >= section)
        )
        second = as_float(lane // CAP % 2 == 1)
        for shift, ref in zip(shifts, part_refs):
            source = (section + sections - shift) % sections
            here = jnp.where(source < sections // 2, 1.0 - second, second) * taken
            near = pl.multiple_of(source % (sections // 2) * part_width, part_width)
            added = matmul(here.astype(BF16), back_ref[:, pl.ds(near, part_width)])
            far = pl.multiple_of(source * part_width, part_width)
            out_ref[:, pl.ds(far, part_width)] = (
                ref[:count, :].astype(F32) + added
            ).astype(BF16)

    shape = (count, 2 * side)
    return pl.pallas_call(
        kernel,
        compiler_params=grant(8),
        in_specs=[pl.BlockSpec(memory_space=pltpu.SMEM)]
        + [whole_spec(value.shape) for value in (tokens, *parts, back)],
        out_specs=whole_spec(shape),
        out_shape=jax.ShapeDtypeStruct(shape, BF16),
    )(where, tokens, *parts, back)


def on_device(saved_inputs, expert_ids, gate_weights, out_grad, gate_w, up_w, down_w):
    sections = lax.axis_size("section")
    devices = lax.axis_size("ep")
    chips = devices // 2
    section = lax.axis_index("section")
    place = lax.axis_index("ep")
    core = place % 2
    groups = [[2 * chip + k for chip in range(chips)] for k in range(2)]
    width = saved_inputs.shape[2]
    columns = width // devices
    slots = devices * CAP
    tokens = saved_inputs[0]
    token_count = tokens.shape[0]
    w_gate = gate_w[0]
    w_up = up_w[0]
    w_down = down_w[0]

    where = jnp.stack([section, core, place]).astype(jnp.int32)
    sent, select, slot_weight = prepare(
        expert_ids[0].T, gate_weights[0].T, out_grad, sections
    )

    def around(value, shift):
        pairs = [(i, (i + shift) % sections) for i in range(sections)]
        return lax.ppermute(value, "section", pairs)

    parts = [sent]
    above = below = sent
    for shift in range(1, sections // 2 + 1):
        below = around(below, 1)
        parts.append(below)
        if shift < sections // 2:
            above = around(above, -1)
            parts.append(above)
    x_mine = exchange(pack_inputs(select, tokens, chips), "ep", groups)
    x_mine, parts, select, slot_weight, where = lax.optimization_barrier(
        (x_mine, parts, select, slot_weight, where)
    )
    x_other = from_partner(x_mine, devices)
    packed, all_tokens = pack(where, parts, select, slot_weight, chips)
    y_mine = exchange(packed, "ep", groups)
    y_other = from_partner(y_mine, devices)
    flat = lambda value: value.reshape(chips * ROWS, value.shape[2])

    (
        feeds_few,
        pick_few,
        weight_few,
        notes,
        column,
        x_rows,
        y_rows,
        act,
        slope,
        hidden,
        gate_first,
        up_first,
        act_few,
        slope_few,
        hidden_few,
        gate_few,
        up_few,
        rows_few,
        y_few,
        share_few,
        fits,
        trips,
    ) = first_pass(
        where,
        flat(x_mine),
        flat(x_other),
        flat(y_mine),
        flat(y_other),
        w_gate,
        w_up,
        w_down,
        sections,
    )
    trips = trips.reshape(())

    def slow_plan(size):
        layer_index = jnp.arange(sections, dtype=jnp.int32)
        index = jnp.arange(size, dtype=jnp.int32)
        in_chain = (notes[:, : sections * CAP] >= 0).reshape(devices, sections, CAP)
        flags = jnp.swapaxes(in_chain, 0, 1).reshape(sections, slots)
        within = notes[:, : sections * CAP].astype(jnp.int32).reshape(devices, sections, CAP)
        base = token_count * jnp.arange(devices, dtype=jnp.int32)[:, None, None]
        token = jnp.swapaxes(within + base + 1, 0, 1).reshape(sections, slots)
        place = jnp.cumsum(flags.astype(jnp.int32), axis=1) - 1
        listed = flags[:, None, :] & (place[:, None, :] == index[None, :, None])
        tokens_of = jnp.sum(jnp.where(listed, token[:, None, :], 0), axis=2)
        own_token = lax.dynamic_index_in_dim(tokens_of, section, 0, keepdims=False)
        own = lax.dynamic_index_in_dim(listed, section, 0, keepdims=False)
        parts = notes[:, sections * CAP : (sections + PARTS) * CAP].reshape(devices, PARTS, CAP)
        weight = jnp.sum(jnp.where(own, jnp.sum(parts, axis=1).reshape(1, slots), 0.0), axis=1)
        feeds = (
            (own_token[:, None, None] == tokens_of[None])
            & (own_token[:, None, None] > 0)
            & (layer_index[None, :, None] > section)
        )
        halves = own.reshape(size, 2, chips, CAP)
        halves = jnp.where(core == 0, halves, halves[:, ::-1])
        halves = jnp.concatenate([halves, jnp.zeros_like(halves)], 3)
        return (
            feeds.reshape(size, sections * size).astype(BF16),
            halves.reshape(size, devices * ROWS).astype(BF16),
            jnp.broadcast_to(weight[:, None], (size, LANES)),
        )

    def slow_start(size):
        feeds, pick, weight = slow_plan(size)
        exact = lambda value: lax.dot_general(
            value,
            pick.astype(F32),
            (((1,), (1,)), ((), ())),
            precision=lax.Precision.HIGHEST,
        )
        gate = project(gate_first, pick).astype(BF16)
        up = project(up_first, pick).astype(BF16)
        share = (sum_rows(gate, w_gate) + sum_rows(up, w_up)).astype(BF16)
        return (
            feeds,
            pick,
            weight,
            exact(act),
            exact(slope),
            project(hidden, pick).astype(BF16),
            gate,
            up,
            matmul(pick, column),
            jnp.zeros((size, width), BF16),
            jnp.swapaxes(share.reshape(size, devices, columns), 0, 1),
        )

    def finish(size):
        if size == FEW:
            start = (
                feeds_few,
                pick_few,
                weight_few,
                act_few,
                slope_few,
                hidden_few,
                gate_few,
                up_few,
                rows_few,
                y_few,
                share_few,
            )
        else:
            start = slow_start(size)
        feeds, pick, weight, act_rows, slope_rows, hidden_rows = start[:6]
        first_rows = start[8]

        def more(state):
            return state[0] < trips

        def step(state):
            trip = state[0] + 1
            last = (trip >= trips).astype(jnp.int32).reshape(1)
            share, trip, last = lax.optimization_barrier((state[4], trip, last))
            summed = jnp.sum(exchange(share, "ep").astype(F32), axis=0)
            high = lax.reduce_precision(summed, 8, 7)
            summed = jnp.concatenate([high.astype(BF16), (summed - high).astype(BF16)], 0)
            layers = exchange(repeated(summed, sections), "section")
            blocks = exchange(chain_rows(layers, feeds, first_rows, weight, devices), "ep")
            y, gate, up, share = chain_step(last, blocks, act_rows, slope_rows, w_gate, w_up, w_down)
            return (trip, y, gate, up, share)

        state = (jnp.int32(0), start[9], start[6], start[7], start[10])
        _, y, gate, up, _ = lax.while_loop(more, step, state)
        gate, up, hidden_kept, share_mine, share_other = merge_chains(
            pick, gate_first, up_first, hidden, gate, up, w_gate, w_up
        )

        theirs = from_partner(share_other, devices)
        chip_sum = (share_mine.astype(F32) + theirs.astype(F32)).astype(BF16)
        tiles = exchange(chip_sum.reshape(chips, ROWS, width // 2), "ep", groups)
        back = lax.reduce_precision(jnp.sum(tiles.astype(F32), axis=0), 8, 7).astype(BF16)
        grads = weight_gradients(
            x_rows, y_rows, gate, up, hidden_kept, hidden_rows, y
        )
        spread, grads = lax.optimization_barrier((repeated(back, sections), grads))
        all_back = exchange(spread, "section")
        result = assemble(where, all_tokens, parts, all_back.reshape(sections * ROWS, width // 2))
        return (result, *grads)

    outputs = lax.cond(fits.reshape(()) != 0, lambda: finish(FEW), lambda: finish(slots))
    return tuple(output[None] for output in outputs)


def solution(mesh):
    by_rows = P("section", "ep", None)
    return jax.shard_map(
        on_device,
        mesh=mesh,
        in_specs=(by_rows, by_rows, by_rows, P("ep", "section"), by_rows, by_rows, by_rows),
        out_specs=(by_rows, by_rows, by_rows, by_rows),
        check_vma=False,
    )
```

```python
import jax
import jax.numpy as jnp
from jax import lax
from jax.experimental import pallas as pl
from jax.experimental.pallas import tpu as pltpu
from jax.sharding import PartitionSpec as P


CAP = 4
ROWS = 2 * CAP
FEW = 16
PARTS = 3
LANES = 128
F32 = jnp.float32
BF16 = jnp.bfloat16


def exchange(blocks, axis, groups=None):
    return lax.all_to_all(blocks, axis, 0, 0, tiled=True, axis_index_groups=groups)


def repeated(value, count):
    return jnp.broadcast_to(value[None], (count, *value.shape))


def from_partner(value, devices):
    return lax.ppermute(value, "ep", [(i, i ^ 1) for i in range(devices)])


def project(row_data, weight):
    return lax.dot_general(
        row_data, weight, (((1,), (1,)), ((), ())), preferred_element_type=F32
    )


def matmul(left, right):
    return jnp.dot(left, right, preferred_element_type=F32)


def sum_rows(left, right):
    return lax.dot_general(
        left, right, (((0,), (0,)), ((), ())), preferred_element_type=F32
    )


def iota(shape, dim):
    return lax.broadcasted_iota(jnp.int32, shape, dim)


def grant(mebibytes):
    return pltpu.CompilerParams(vmem_limit_bytes=mebibytes << 20)


def as_float(mask):
    return jnp.where(mask, 1.0, 0.0)


def whole_spec(shape):
    return pl.BlockSpec(shape, lambda: (0,) * len(shape))


def first_pass(where, x_mine, x_other, mine, other, w_gate, w_up, w_down, sections):
    half = mine.shape[0] // ROWS
    rows = half * ROWS
    side = x_mine.shape[1]
    devices = 2 * half
    codes = sections * CAP
    ending = codes + PARTS * CAP
    units, width = w_gate.shape
    columns = width // devices

    def kernel(
        where_ref,
        x_mine_ref,
        x_other_ref,
        mine_ref,
        other_ref,
        w_gate_ref,
        w_up_ref,
        w_down_ref,
        feeds_ref,
        pick_ref,
        weight_ref,
        note_ref,
        column_ref,
        rows_ref,
        scaled_ref,
        act_ref,
        slope_ref,
        hidden_ref,
        gate_ref,
        up_ref,
        act_few_ref,
        slope_few_ref,
        hidden_few_ref,
        gate_few_ref,
        up_few_ref,
        rows_few_ref,
        y_few_ref,
        share_ref,
        fits_ref,
        trips_ref,
    ):
        section = where_ref[0]
        core = where_ref[1]
        place = where_ref[2]

        lead = as_float(iota((half, rows), 1) == ROWS * iota((half, rows), 0)).astype(BF16)
        tiles = [ref[:, side:] for ref in (mine_ref, other_ref)]
        near = matmul(lead, tiles[0])
        far = matmul(lead, tiles[1])
        note = jnp.concatenate([jnp.where(core == 0, near, far), jnp.where(core == 0, far, near)], 0)
        note_ref[...] = note
        lane = iota((devices, LANES), 1)
        code = jnp.where(lane < codes, note, -1.0)
        flag = as_float(code >= 0)
        row = iota((LANES, LANES), 0)
        col = iota((LANES, LANES), 1)
        same_layer = row // CAP == col // CAP
        per_layer = matmul(flag, as_float(same_layer))
        longest = jnp.max(jnp.sum(per_layer, axis=0, keepdims=True))
        fits_ref[0] = (longest <= FEW).astype(jnp.int32)
        most = jnp.max(jnp.where(lane == codes + PARTS * CAP, note, 0.0))
        trips_ref[0] = most.astype(jnp.int32) - 1
        before = as_float(iota((devices, devices), 1) < iota((devices, devices), 0))
        rank = matmul(before, per_layer) + matmul(flag, as_float(same_layer & (row < col)))
        rank = (rank + 1.0) * flag
        token = (code + 1.0) * flag
        owned = as_float(iota((8, LANES), 1) == iota((8, LANES), 0) + CAP * section)
        own_rank = project(owned, rank)
        own_token = project(owned, token)
        entry = iota((FEW, devices), 0).astype(F32) + 1.0
        device = iota((devices, 2 * rows), 0)
        spot = iota((devices, 2 * rows), 1)
        home = rows * ((device // half + core) % 2) + ROWS * (device % half)
        held = jnp.zeros((FEW, 1), F32)
        weight = jnp.zeros((FEW, LANES), F32)
        groups = jnp.zeros((FEW, devices), F32)
        pick = jnp.zeros((FEW, 2 * rows), F32)
        few_lane = iota((FEW, LANES), 1)
        for slot in range(CAP):
            here = as_float(own_rank[slot : slot + 1] == entry)
            groups = groups + here
            held = held + jnp.sum(here * own_token[slot : slot + 1], axis=1, keepdims=True)
            part = matmul(here, note)
            wanted = (few_lane >= codes) & (few_lane < ending) & (few_lane % CAP == slot)
            weight = weight + jnp.where(wanted, part, 0.0)
            pick = pick + matmul(here, as_float(spot == home + slot))
        near_rank = matmul(groups, rank)
        near_token = matmul(groups, token)
        match = (near_token == held) & (near_token > 0) & (few_lane // CAP > section)
        source = jnp.where(match & (few_lane < codes), near_rank, 0.0)
        feeds = jnp.zeros((FEW, LANES), F32)
        for slot in range(CAP):
            spread = as_float((row // CAP == col // FEW) & (row % CAP == slot))
            feeds = feeds + as_float(
                matmul(source, spread) == (few_lane % FEW + 1).astype(F32)
            )
        feeds_ref[...] = feeds.astype(BF16)
        pick_low = pick.astype(BF16)
        pick_ref[...] = pick_low
        weight_ref[...] = jnp.broadcast_to(
            jnp.sum(weight, axis=1, keepdims=True), (FEW, LANES)
        )

        tile_row = iota((rows, LANES), 0)
        tile_lane = iota((rows, LANES), 1)
        wanted = (tile_lane >= codes) & (tile_lane < ending) & (tile_lane % CAP == tile_row % CAP)
        for index, ref in enumerate((mine_ref, other_ref)):
            scale = jnp.sum(
                jnp.where(wanted, tiles[index].astype(F32), 0.0), axis=1, keepdims=True
            )
            part = slice(index * rows, (index + 1) * rows)
            scaled_ref[part, :] = (ref[:, :side].astype(F32) * scale).astype(BF16)
            rows_ref[part, :] = (x_mine_ref, x_other_ref)[index][...]
        y_few_ref[...] = jnp.zeros((FEW, width), BF16)
        blocks = side // columns
        spot = pl.ds(pl.multiple_of(place % blocks * columns, columns), columns)
        column = jnp.concatenate([mine_ref[:, spot], other_ref[:, spot]], 0).astype(F32)
        column = jnp.where(place < blocks, column, pltpu.roll(column, 2 * rows - CAP, 0))
        column_ref[...] = column.astype(BF16)
        rows_few_ref[...] = matmul(pick_low, column_ref[...])
        x_lane = iota((units, 2 * rows), 1) % ROWS < CAP

        def whole_rows(weight_ref, ref):
            return project(weight_ref[:, :side], ref[...]) + pltpu.roll(
                project(weight_ref[:, side:], ref[...]), 2 * rows - CAP, 1
            )

        grad = whole_rows(w_down_ref, scaled_ref)
        gate_pre = whole_rows(w_gate_ref, rows_ref)
        up_pre = whole_rows(w_up_ref, rows_ref)
        sig = 1.0 / (1.0 + jnp.exp(-gate_pre))
        act = jnp.where(x_lane, gate_pre * sig, 0.0)
        slope = jnp.where(x_lane, up_pre * sig * (1.0 + gate_pre * (1.0 - sig)), 0.0)
        act_ref[...] = act
        slope_ref[...] = slope
        hidden_ref[...] = (act * up_pre).astype(BF16)
        gate_ref[...] = (grad * slope).astype(BF16)
        up_ref[...] = (grad * act).astype(BF16)

        def exact(value):
            total = jnp.zeros((units, FEW), F32)
            for _ in range(PARTS):
                piece = value.astype(BF16)
                total = total + project(piece, pick_low)
                value = value - piece.astype(F32)
            return total

        act_few_ref[...] = exact(act_ref[...])
        slope_few_ref[...] = exact(slope_ref[...])
        hidden_few_ref[...] = project(hidden_ref[...], pick_low).astype(BF16)
        gate_few = project(gate_ref[...], pick_low).astype(BF16)
        up_few = project(up_ref[...], pick_low).astype(BF16)
        gate_few_ref[...] = gate_few
        up_few_ref[...] = up_few
        share = (sum_rows(gate_few, w_gate_ref[...]) + sum_rows(up_few, w_up_ref[...])).astype(BF16)
        for index in range(devices):
            share_ref[index] = share[:, index * columns : (index + 1) * columns]

    shapes = [
        ((FEW, sections * FEW), BF16),
        ((FEW, ROWS * devices), BF16),
        ((FEW, LANES), F32),
        ((devices, LANES), F32),
        ((2 * rows, columns), BF16),
        ((2 * rows, side), BF16),
        ((2 * rows, side), BF16),
        ((units, 2 * rows), F32),
        ((units, 2 * rows), F32),
        ((units, 2 * rows), BF16),
        ((units, 2 * rows), BF16),
        ((units, 2 * rows), BF16),
        ((units, FEW), F32),
        ((units, FEW), F32),
        ((units, FEW), BF16),
        ((units, FEW), BF16),
        ((units, FEW), BF16),
        ((FEW, columns), F32),
        ((FEW, width), BF16),
        ((devices, FEW, columns), BF16),
    ]
    smem = pl.BlockSpec(memory_space=pltpu.SMEM)
    return pl.pallas_call(
        kernel,
        compiler_params=grant(28),
        in_specs=[smem] + [whole_spec(value.shape) for value in (x_mine, x_other, mine, other)] + [whole_spec(w_gate.shape)] * 3,
        out_specs=[whole_spec(shape) for shape, _ in shapes] + [smem] * 2,
        out_shape=[jax.ShapeDtypeStruct(shape, dtype) for shape, dtype in shapes]
        + [jax.ShapeDtypeStruct((1,), jnp.int32)] * 2,
    )(where, x_mine, x_other, mine, other, w_gate, w_up, w_down)


def chain_rows(layers, feeds, first_rows, weight, devices):
    sections = layers.shape[0]
    size, columns = first_rows.shape

    def kernel(layers_ref, feeds_ref, first_ref, weight_ref, out_ref):
        rows = first_ref[...]
        for layer in range(sections - 1, 0, -1):
            feed = feeds_ref[:, layer * size : (layer + 1) * size]
            added = matmul(feed, layers_ref[layer, :size, :]) + matmul(
                feed, layers_ref[layer, size:, :]
            )
            rows = (rows + added).astype(BF16).astype(F32)
        rows = (weight_ref[...] * rows).astype(BF16)
        for device in range(devices):
            out_ref[device] = rows

    values = (layers, feeds, first_rows, weight)
    shape = (devices, size, columns)
    return pl.pallas_call(
        kernel,
        compiler_params=grant(8),
        in_specs=[whole_spec(value.shape) for value in values],
        out_specs=whole_spec(shape),
        out_shape=jax.ShapeDtypeStruct(shape, BF16),
    )(*values)


def chain_step(last, y_blocks, act_few, slope_few, w_gate, w_up, w_down):
    devices, size, columns = y_blocks.shape
    units, width = w_gate.shape

    def kernel(
        last_ref,
        blocks_ref,
        act_ref,
        slope_ref,
        gate_hbm,
        up_hbm,
        w_down_ref,
        y_ref,
        gate_few_ref,
        up_few_ref,
        share_ref,
        w_gate_ref,
        w_up_ref,
        sems,
    ):
        copies = [
            pltpu.make_async_copy(gate_hbm, w_gate_ref, sems.at[0]),
            pltpu.make_async_copy(up_hbm, w_up_ref, sems.at[1]),
        ]

        @pl.when(last_ref[0] == 0)
        def _():
            for copy in copies:
                copy.start()

        for index in range(devices):
            y_ref[:, index * columns : (index + 1) * columns] = blocks_ref[index]
        grad = project(w_down_ref[...], y_ref[...])
        gate_few = (grad * slope_ref[...]).astype(BF16)
        up_few = (grad * act_ref[...]).astype(BF16)
        gate_few_ref[...] = gate_few
        up_few_ref[...] = up_few

        @pl.when(last_ref[0] == 0)
        def _():
            for copy in copies:
                copy.wait()
            share = sum_rows(gate_few, w_gate_ref[...])
            share = (share + sum_rows(up_few, w_up_ref[...])).astype(BF16)
            for index in range(devices):
                share_ref[index] = share[:, index * columns : (index + 1) * columns]

    shapes = [(size, width), (units, size), (units, size), (devices, size, columns)]
    return pl.pallas_call(
        kernel,
        compiler_params=grant(16),
        in_specs=[pl.BlockSpec(memory_space=pltpu.SMEM)]
        + [whole_spec(value.shape) for value in (y_blocks, act_few, slope_few)]
        + [pl.BlockSpec(memory_space=pl.ANY)] * 2
        + [whole_spec(w_down.shape)],
        out_specs=[whole_spec(shape) for shape in shapes],
        out_shape=[jax.ShapeDtypeStruct(shape, BF16) for shape in shapes],
        scratch_shapes=[
            pltpu.VMEM(w_gate.shape, BF16),
            pltpu.VMEM(w_up.shape, BF16),
            pltpu.SemaphoreType.DMA((2,)),
        ],
    )(last, y_blocks, act_few, slope_few, w_gate, w_up, w_down)


def merge_chains(pick, gate, up, hidden, gate_few, up_few, w_gate, w_up):
    units, width = w_gate.shape
    lanes = gate.shape[1]
    rows = lanes // 2

    def kernel(
        pick_ref,
        gate_ref,
        up_ref,
        hidden_ref,
        gate_few_ref,
        up_few_ref,
        w_gate_ref,
        w_up_ref,
        gate_out,
        up_out,
        hidden_out,
        mine_out,
        other_out,
    ):
        pick_low = pick_ref[...]
        keep = jnp.sum(pick_low.astype(F32), axis=0, keepdims=True) == 0.0
        gate_all = jnp.where(keep, gate_ref[...].astype(F32), matmul(gate_few_ref[...], pick_low))
        up_all = jnp.where(keep, up_ref[...].astype(F32), matmul(up_few_ref[...], pick_low))
        kept = jnp.where(keep, hidden_ref[...].astype(F32), 0.0)
        for ref, value in ((gate_out, gate_all), (up_out, up_all), (hidden_out, kept)):
            ref[0] = value.astype(BF16)
            ref[1] = pltpu.roll(value, CAP, 1).astype(BF16)
        side = width // 2

        def shares(ref, weight_ref):
            return sum_rows(ref[0], weight_ref[:, :side]) + sum_rows(ref[1], weight_ref[:, side:])

        share = (shares(gate_out, w_gate_ref) + shares(up_out, w_up_ref)).astype(BF16)
        mine_out[...] = share[:rows]
        other_out[...] = share[rows:]

    shapes = [(2, units, lanes)] * 3 + [(rows, width // 2)] * 2
    values = (pick, gate, up, hidden, gate_few, up_few)
    return pl.pallas_call(
        kernel,
        compiler_params=grant(16),
        in_specs=[whole_spec(value.shape) for value in values] + [whole_spec(w_gate.shape)] * 2,
        out_specs=[whole_spec(shape) for shape in shapes],
        out_shape=[jax.ShapeDtypeStruct(shape, BF16) for shape in shapes],
    )(*values, w_gate, w_up)


def weight_gradients(x_rows, y_rows, gate, up, hidden, hidden_few, y_few):
    _, units, lanes = gate.shape
    few, width = y_few.shape
    block = 512
    per_side = x_rows.shape[1] // block

    def kernel(x_ref, y_ref, gate_ref, up_ref, h_ref, hf_ref, yf_ref, gate_out, up_out, down_out):
        gate_out[...] = matmul(gate_ref[0], x_ref[...]).astype(BF16)
        up_out[...] = matmul(up_ref[0], x_ref[...]).astype(BF16)
        down_out[...] = (
            matmul(h_ref[0], y_ref[...]) + matmul(hf_ref[...], yf_ref[...])
        ).astype(BF16)

    half = pl.BlockSpec((1, units, lanes), lambda i: (i // per_side, 0, 0))
    side = pl.BlockSpec((lanes, block), lambda i: (0, i % per_side))
    across = lambda count: pl.BlockSpec((count, block), lambda i: (0, i))
    return pl.pallas_call(
        kernel,
        compiler_params=grant(16),
        grid=(width // block,),
        in_specs=[side, side, half, half, half]
        + [pl.BlockSpec(hidden_few.shape, lambda i: (0, 0)), across(few)],
        out_specs=[across(units)] * 3,
        out_shape=[jax.ShapeDtypeStruct((units, width), BF16)] * 3,
    )(x_rows, y_rows, gate, up, hidden, hidden_few, y_few)


def prepare(ids, weights, out_grad, sections):
    count, part_width = out_grad.shape
    codes = sections * CAP

    def kernel(ids_ref, weights_ref, grad_ref, sent_ref, select_ref, weight_ref):
        live = as_float(ids_ref[...] == 0)
        weight = jnp.sum(live * weights_ref[...], axis=0, keepdims=True)
        live = jnp.sum(live, axis=0, keepdims=True)
        row = iota((count, count), 0)
        col = iota((count, count), 1)
        slot = matmul(jnp.broadcast_to(live, (8, count)), as_float(row < col))[:1]
        slot = jnp.where(live > 0, slot, -1.0)
        at_slot = as_float(slot == row.astype(F32))
        index = iota((8, count), 1).astype(F32) + 1.0
        token = project(index, at_slot) - 1.0
        tile = jnp.concatenate([token, jnp.zeros((8, part_width - count), F32)], 1).astype(BF16)
        sent_ref[:count, :] = grad_ref[...]
        sent_ref[count:, :] = tile
        select_ref[...] = at_slot[:8].astype(BF16)
        parts = jnp.zeros((8, LANES), F32)
        remainder = weight
        for part in range(PARTS):
            piece = remainder.astype(BF16).astype(F32)
            remainder = remainder - piece
            moved = as_float((slot + (codes + part * CAP) == row.astype(F32)) & (slot >= 0))
            parts = parts + project(jnp.broadcast_to(piece, (8, count)), moved)
        weight_ref[...] = parts

    shapes = [((count + 8, part_width), BF16), ((8, count), BF16), ((8, LANES), F32)]
    return pl.pallas_call(
        kernel,
        compiler_params=grant(8),
        in_specs=[whole_spec(value.shape) for value in (ids, weights, out_grad)],
        out_specs=[whole_spec(shape) for shape, _ in shapes],
        out_shape=[jax.ShapeDtypeStruct(shape, dtype) for shape, dtype in shapes],
    )(ids, weights, out_grad)


def halves_of(select):
    low = select.astype(F32)
    return low, pltpu.roll(low, CAP, 0)


def pack_inputs(select, tokens, chips):
    side = tokens.shape[1] // 2

    def kernel(select_ref, tokens_ref, packed_ref):
        low, high = halves_of(select_ref[...])
        rows = (
            matmul(low.astype(BF16), tokens_ref[:, :side])
            + matmul(high.astype(BF16), tokens_ref[:, side:])
        ).astype(BF16)
        for chip in range(chips):
            packed_ref[chip] = rows

    shape = (chips, ROWS, side)
    return pl.pallas_call(
        kernel,
        compiler_params=grant(8),
        in_specs=[whole_spec(select.shape), whole_spec(tokens.shape)],
        out_specs=whole_spec(shape),
        out_shape=jax.ShapeDtypeStruct(shape, BF16),
    )(select, tokens)


def shifts_of(sections):
    return [0] + [way * d for d in range(1, sections // 2) for way in (1, -1)] + [sections // 2]


def pack(where, parts, select, weight, chips):
    sections = len(parts)
    tall, part_width = parts[0].shape
    count = tall - 8
    side = sections * part_width // 2
    codes = sections * CAP
    shifts = shifts_of(sections)

    def kernel(where_ref, *refs):
        part_refs = refs[:sections]
        select_ref, weight_ref, packed_ref, token_ref, rows_ref, tokens_ref = refs[sections:]
        section = where_ref[0]
        low, high = halves_of(select_ref[...])
        rows_ref[...] = jnp.zeros((ROWS, side), F32)
        for shift, ref in zip(shifts, part_refs):
            source = (section + sections - shift) % sections
            chosen = jnp.where(source < sections // 2, low, high).astype(BF16)
            start = source % (sections // 2) * part_width
            spot = pl.ds(pl.multiple_of(start, part_width), part_width)
            rows_ref[:, spot] += matmul(chosen, ref[:count, :])
            tokens_ref[pl.ds(source, 1), :] = ref[count:, :LANES].astype(F32)[:1]
        tokens = tokens_ref[...]
        row = iota((LANES, LANES), 0)
        col = iota((LANES, LANES), 1)
        spread = matmul(tokens, as_float((row < CAP) & (col % CAP == row)))
        lane = iota((sections, LANES), 1)
        layer = iota((sections, LANES), 0)
        pick_lane = lambda size: jnp.sum(
            jnp.where(lane // size == layer, spread, 0.0), axis=0, keepdims=True
        )
        flat = pick_lane(CAP)
        one_lane = lane[:1]
        flat = jnp.where(one_lane < codes, flat, -1.0)
        times = jnp.zeros((1, LANES), F32)
        for slot in range(CAP):
            times = times + jnp.sum(
                as_float(tokens[:, slot : slot + 1] == flat), axis=0, keepdims=True
            )
        times = jnp.where(flat >= 0, times, 0.0)
        code = jnp.where(times > 1, flat, -1.0)
        note = jnp.where(one_lane < codes, code, weight_ref[:1])
        note = jnp.where(one_lane == codes + PARTS * CAP, jnp.max(times), note)
        note = jnp.broadcast_to(note, (ROWS, LANES)).astype(BF16)
        token_ref[...] = jnp.broadcast_to(pick_lane(2 * CAP), (8, LANES))
        rows = rows_ref[...].astype(BF16)
        for chip in range(chips):
            packed_ref[chip, :, :side] = rows
            packed_ref[chip, :, side:] = note

    shapes = [((chips, ROWS, side + LANES), BF16), ((8, LANES), F32)]
    return pl.pallas_call(
        kernel,
        compiler_params=grant(8),
        in_specs=[pl.BlockSpec(memory_space=pltpu.SMEM)]
        + [whole_spec(value.shape) for value in (*parts, select, weight)],
        out_specs=[whole_spec(shape) for shape, _ in shapes],
        out_shape=[jax.ShapeDtypeStruct(shape, dtype) for shape, dtype in shapes],
        scratch_shapes=[pltpu.VMEM((ROWS, side), F32), pltpu.VMEM((sections, LANES), F32)],
    )(where, *parts, select, weight)


def assemble(where, tokens, parts, back):
    sections = len(parts)
    tall, part_width = parts[0].shape
    count = tall - 8
    rows, side = back.shape
    shifts = shifts_of(sections)

    def kernel(where_ref, token_ref, *refs):
        part_refs = refs[:sections]
        back_ref, out_ref = refs[sections:]
        section = where_ref[0]
        lane = iota((count, rows), 1)
        taken = as_float(
            (token_ref[:1, :rows] == iota((count, rows), 0).astype(F32))
            & (lane // (2 * CAP) >= section)
        )
        second = as_float(lane // CAP % 2 == 1)
        for shift, ref in zip(shifts, part_refs):
            source = (section + sections - shift) % sections
            here = jnp.where(source < sections // 2, 1.0 - second, second) * taken
            near = pl.multiple_of(source % (sections // 2) * part_width, part_width)
            added = matmul(here.astype(BF16), back_ref[:, pl.ds(near, part_width)])
            far = pl.multiple_of(source * part_width, part_width)
            out_ref[:, pl.ds(far, part_width)] = (
                ref[:count, :].astype(F32) + added
            ).astype(BF16)

    shape = (count, 2 * side)
    return pl.pallas_call(
        kernel,
        compiler_params=grant(8),
        in_specs=[pl.BlockSpec(memory_space=pltpu.SMEM)]
        + [whole_spec(value.shape) for value in (tokens, *parts, back)],
        out_specs=whole_spec(shape),
        out_shape=jax.ShapeDtypeStruct(shape, BF16),
    )(where, tokens, *parts, back)


def on_device(saved_inputs, expert_ids, gate_weights, out_grad, gate_w, up_w, down_w):
    sections = lax.axis_size("section")
    devices = lax.axis_size("ep")
    chips = devices // 2
    section = lax.axis_index("section")
    place = lax.axis_index("ep")
    core = place % 2
    groups = [[2 * chip + k for chip in range(chips)] for k in range(2)]
    width = saved_inputs.shape[2]
    columns = width // devices
    slots = devices * CAP
    tokens = saved_inputs[0]
    token_count = tokens.shape[0]
    w_gate = gate_w[0]
    w_up = up_w[0]
    w_down = down_w[0]

    where = jnp.stack([section, core, place]).astype(jnp.int32)
    sent, select, slot_weight = prepare(
        expert_ids[0].T, gate_weights[0].T, out_grad, sections
    )

    def around(value, shift):
        pairs = [(i, (i + shift) % sections) for i in range(sections)]
        return lax.ppermute(value, "section", pairs)

    parts = [sent]
    above = below = sent
    for shift in range(1, sections // 2 + 1):
        below = around(below, 1)
        parts.append(below)
        if shift < sections // 2:
            above = around(above, -1)
            parts.append(above)
    x_mine = exchange(pack_inputs(select, tokens, chips), "ep", groups)
    x_mine, parts, select, slot_weight, where = lax.optimization_barrier(
        (x_mine, parts, select, slot_weight, where)
    )
    x_other = from_partner(x_mine, devices)
    packed, all_tokens = pack(where, parts, select, slot_weight, chips)
    y_mine = exchange(packed, "ep", groups)
    y_other = from_partner(y_mine, devices)
    flat = lambda value: value.reshape(chips * ROWS, value.shape[2])

    (
        feeds_few,
        pick_few,
        weight_few,
        notes,
        column,
        x_rows,
        y_rows,
        act,
        slope,
        hidden,
        gate_first,
        up_first,
        act_few,
        slope_few,
        hidden_few,
        gate_few,
        up_few,
        rows_few,
        y_few,
        share_few,
        fits,
        trips,
    ) = first_pass(
        where,
        flat(x_mine),
        flat(x_other),
        flat(y_mine),
        flat(y_other),
        w_gate,
        w_up,
        w_down,
        sections,
    )
    trips = trips.reshape(())

    def slow_plan(size):
        layer_index = jnp.arange(sections, dtype=jnp.int32)
        index = jnp.arange(size, dtype=jnp.int32)
        in_chain = (notes[:, : sections * CAP] >= 0).reshape(devices, sections, CAP)
        flags = jnp.swapaxes(in_chain, 0, 1).reshape(sections, slots)
        within = notes[:, : sections * CAP].astype(jnp.int32).reshape(devices, sections, CAP)
        base = token_count * jnp.arange(devices, dtype=jnp.int32)[:, None, None]
        token = jnp.swapaxes(within + base + 1, 0, 1).reshape(sections, slots)
        place = jnp.cumsum(flags.astype(jnp.int32), axis=1) - 1
        listed = flags[:, None, :] & (place[:, None, :] == index[None, :, None])
        tokens_of = jnp.sum(jnp.where(listed, token[:, None, :], 0), axis=2)
        own_token = lax.dynamic_index_in_dim(tokens_of, section, 0, keepdims=False)
        own = lax.dynamic_index_in_dim(listed, section, 0, keepdims=False)
        parts = notes[:, sections * CAP : (sections + PARTS) * CAP].reshape(devices, PARTS, CAP)
        weight = jnp.sum(jnp.where(own, jnp.sum(parts, axis=1).reshape(1, slots), 0.0), axis=1)
        feeds = (
            (own_token[:, None, None] == tokens_of[None])
            & (own_token[:, None, None] > 0)
            & (layer_index[None, :, None] > section)
        )
        halves = own.reshape(size, 2, chips, CAP)
        halves = jnp.where(core == 0, halves, halves[:, ::-1])
        halves = jnp.concatenate([halves, jnp.zeros_like(halves)], 3)
        return (
            feeds.reshape(size, sections * size).astype(BF16),
            halves.reshape(size, devices * ROWS).astype(BF16),
            jnp.broadcast_to(weight[:, None], (size, LANES)),
        )

    def slow_start(size):
        feeds, pick, weight = slow_plan(size)
        exact = lambda value: lax.dot_general(
            value,
            pick.astype(F32),
            (((1,), (1,)), ((), ())),
            precision=lax.Precision.HIGHEST,
        )
        gate = project(gate_first, pick).astype(BF16)
        up = project(up_first, pick).astype(BF16)
        share = (sum_rows(gate, w_gate) + sum_rows(up, w_up)).astype(BF16)
        return (
            feeds,
            pick,
            weight,
            exact(act),
            exact(slope),
            project(hidden, pick).astype(BF16),
            gate,
            up,
            matmul(pick, column),
            jnp.zeros((size, width), BF16),
            jnp.swapaxes(share.reshape(size, devices, columns), 0, 1),
        )

    def finish(size):
        if size == FEW:
            start = (
                feeds_few,
                pick_few,
                weight_few,
                act_few,
                slope_few,
                hidden_few,
                gate_few,
                up_few,
                rows_few,
                y_few,
                share_few,
            )
        else:
            start = slow_start(size)
        feeds, pick, weight, act_rows, slope_rows, hidden_rows = start[:6]
        first_rows = start[8]

        def more(state):
            return state[0] < trips

        def step(state):
            trip = state[0] + 1
            last = (trip >= trips).astype(jnp.int32).reshape(1)
            share, trip, last = lax.optimization_barrier((state[4], trip, last))
            summed = jnp.sum(exchange(share, "ep").astype(F32), axis=0)
            high = lax.reduce_precision(summed, 8, 7)
            summed = jnp.concatenate([high.astype(BF16), (summed - high).astype(BF16)], 0)
            layers = exchange(repeated(summed, sections), "section")
            blocks = exchange(chain_rows(layers, feeds, first_rows, weight, devices), "ep")
            y, gate, up, share = chain_step(last, blocks, act_rows, slope_rows, w_gate, w_up, w_down)
            return (trip, y, gate, up, share)

        state = (jnp.int32(0), start[9], start[6], start[7], start[10])
        _, y, gate, up, _ = lax.while_loop(more, step, state)
        gate, up, hidden_kept, share_mine, share_other = merge_chains(
            pick, gate_first, up_first, hidden, gate, up, w_gate, w_up
        )

        theirs = from_partner(share_other, devices)
        chip_sum = (share_mine.astype(F32) + theirs.astype(F32)).astype(BF16)
        tiles = exchange(chip_sum.reshape(chips, ROWS, width // 2), "ep", groups)
        back = lax.reduce_precision(jnp.sum(tiles.astype(F32), axis=0), 8, 7).astype(BF16)
        grads = weight_gradients(
            x_rows, y_rows, gate, up, hidden_kept, hidden_rows, y
        )
        spread, grads = lax.optimization_barrier((repeated(back, sections), grads))
        all_back = exchange(spread, "section")
        result = assemble(where, all_tokens, parts, all_back.reshape(sections * ROWS, width // 2))
        return (result, *grads)

    outputs = lax.cond(fits.reshape(()) != 0, lambda: finish(FEW), lambda: finish(slots))
    return tuple(output[None] for output in outputs)


def solution(mesh):
    by_rows = P("section", "ep", None)
    return jax.shard_map(
        on_device,
        mesh=mesh,
        in_specs=(by_rows, by_rows, by_rows, P("ep", "section"), by_rows, by_rows, by_rows),
        out_specs=(by_rows, by_rows, by_rows, by_rows),
        check_vma=False,
    )
```
